32 devices in a mesh: gx: 4 (over y, core), gy: 2 (over x), gz: 4 (over z).
Axes of the slice: x: 2, y: 2, z: 4, core: 2. Of those that a mesh axis runs over, the one named last changes fastest.
Arguments:
- source: float32 [256, 128, 128], P('gx', 'gy', 'gz'), may hold values from -6 to 6
- green: float32 [512, 256, 256], P(None, ('gx', 'gz'), 'gy'), may hold values from 0.05 to 2, as said below
Outputs:
- potential: float32 [256, 128, 128], P('gx', 'gy', 'gz')
The draws below stay inside these ranges and needn't reach their ends.
Inputs may be any that keep to these rules, and one draw needn't show every extreme that they name: `green`: greenfull is even: greenfull[k] equals greenfull at (-k1 mod 512, -k2 mod 256, -k3 mod 256).
All inputs are finite; a program needn't handle non-finite values.
Results may differ from the reference program's by a relative error of at most 0.00007.
Values sent between devices are 32-bit elements; how exact they have to be, the bound alone decides.
A program may use at most 128 MiB of HBM per device.

```python
import math
import jax
import jax.numpy as jnp

NX = 256
NY = 128
NZ = 128
LX = 512
LY = 256
LZ = 256


def pair_frequency(length):
    position = jnp.arange(length, dtype=jnp.int32)
    unit_index = position // 2
    member = position % 2
    return jnp.where(unit_index == 0, member * (length // 2), jnp.where(member == 0, unit_index, length - unit_index)).astype(jnp.int32)


def draw_green(key, part):
    lower_end = 0.05
    upper_end = 2.0
    drawn = jnp.exp(jax.random.uniform(key, (LX, LY, LZ), jnp.float32, math.log(lower_end), math.log(upper_end)))
    mirrored = jnp.roll(jnp.flip(drawn, (0, 1, 2)), (1, 1, 1), (0, 1, 2))
    symmetric = 0.5 * (drawn + mirrored)
    ordered = jnp.take(symmetric, pair_frequency(LY), axis=1)
    return jnp.take(ordered, pair_frequency(LZ), axis=2)


def level_of(rng, shape, cuts, smallest, top_value):
    factor_of, own = 1.0, jax.random.fold_in(rng, 6)
    for axis_at, shards_of in cuts:
        heights = jnp.exp(jax.random.uniform(jax.random.fold_in(own, axis_at), (shards_of,), jnp.float32, smallest / len(cuts), top_value / len(cuts)))
        factor_of = factor_of * jnp.repeat(heights, shape[axis_at] // shards_of).reshape([-1 if axis == axis_at else 1 for axis in range(len(shape))])
    return factor_of


def centred(stream_key, shape, spread, bound, shards=(), kind=jnp.bfloat16):
    entries = spread * jax.random.normal(stream_key, shape, jnp.float32)
    if shards:
        entries = entries * level_of(stream_key, shape, shards, -0.22, 0.18)
    return jnp.clip(entries, -bound, bound).astype(kind)


def setup_inputs(seed: int = 0) -> dict:
    key_list = jax.random.split(jax.random.key(seed), 3)
    source = centred(key_list[0], (NX, NY, NZ), 1.0, 6.0, ((0, 4), (1, 2), (2, 4)), jnp.float32)
    green = draw_green(jax.random.fold_in(key_list[2], 71), 0)
    return {"source": source, "green": green}


def pair_position(length):
    freq = jnp.arange(length, dtype=jnp.int32)
    half = length // 2
    return jnp.where(freq == 0, 0, jnp.where(freq == half, 1, jnp.where(freq < half, 2 * freq, 2 * (length - freq) + 1))).astype(jnp.int32)


def reference(source, green):
    natural = jnp.take(green, pair_position(LY), axis=1)
    natural = jnp.take(natural, pair_position(LZ), axis=2)
    padded = jnp.pad(source, ((0, NX), (0, NY), (0, NZ)))
    spectrum = jnp.fft.fftn(padded)
    inverse = jnp.fft.ifftn(spectrum * natural)
    return jnp.real(inverse)[:NX, :NY, :NZ].astype(jnp.float32)
```

```python
import functools
import math

import jax
import jax.numpy as jnp
import ml_dtypes
import numpy as np
from jax import lax
from jax.experimental import pallas as pl
from jax.experimental.pallas import tpu as pltpu
from jax.sharding import PartitionSpec as P

LANES = 128
PARTS = 2
CHUNKS = 2
VMEM_BYTES = 48 * 1024 * 1024


def np_halves(table):
    high = table.astype(np.float32).astype(ml_dtypes.bfloat16)
    low = (table - high.astype(np.float64)).astype(np.float32).astype(ml_dtypes.bfloat16)
    return np.stack([high, low])


def split(value):
    high = value.astype(jnp.bfloat16)
    return high, (value - high.astype(jnp.float32)).astype(jnp.bfloat16)


def mm(left, right):
    return jnp.dot(left, right, preferred_element_type=jnp.float32)


def table_left(high, low, value):
    v_high, v_low = split(value)
    both = mm(high, jnp.concatenate([v_high, v_low], axis=1))
    width = value.shape[1]
    return both[:, :width] + (both[:, width:] + mm(low, v_high))


def table_right(value, high, low):
    v_high, v_low = split(value)
    return mm(v_high, high) + (mm(v_low, high) + mm(v_high, low))


def block_swap(pieces, width):
    count = len(pieces)
    group = lax.broadcasted_iota(jnp.int32, pieces[0].shape, 1) // width
    out = []
    for c in range(count):
        total = None
        for g in range(count):
            moved = pieces[g]
            shift = (g - c) * width % LANES
            if shift:
                moved = pltpu.roll(moved, shift, 1)
            total = moved if total is None else jnp.where(group == g, moved, total)
        out.append(total)
    return out


def y_tables(length_y, blocks, units, scale):
    cells = np.arange(length_y // 2)
    freq = np.arange(length_y // 2)
    angle = 2.0 * np.pi * (np.outer(freq, cells) % length_y) / length_y
    sign = 1.0 - 2.0 * (cells % 2)
    real, imag = np.cos(angle), -np.sin(angle)
    imag[0] = sign
    weight = np.where(freq == 0, 1.0, 2.0)[:, None] * (scale / length_y)
    both = np.stack([real, imag], axis=1)
    back = both * weight[:, None]

    def ordered(table):
        table = table.reshape(blocks, 2, PARTS, units // PARTS, 2, -1)
        return table.transpose(1, 2, 0, 3, 4, 5).reshape(2, length_y // 2, -1)

    forward = np.swapaxes(np_halves(ordered(both)), 0, 1)
    backward = np.swapaxes(np_halves(np.swapaxes(ordered(back), 1, 2)), 0, 1)
    return forward, backward


def x_table(length_x, group, rows):
    freqs = np.arange(length_x // 4)
    place = np.arange(length_x // 4)
    block, rest = place // (group * rows), place % (group * rows)
    cells = block * group * rows + rest % rows * group + rest // rows
    out = []
    for member in range(4):
        freq = 4 * freqs + member
        angle = 2.0 * np.pi * (np.outer(freq, cells) % length_x) / length_x
        out.append(np.concatenate([np.cos(angle), np.sin(angle)], 1))
    return np_halves(np.stack(out))


def z_table(length_z, parts):
    place = np.arange(length_z)
    unit, member = place // 2, place % 2
    freq = np.where(unit == 0, member * (length_z // 2), np.where(member == 0, unit, length_z - unit))
    cells = np.arange(length_z // 2)
    rows = []
    for freqs in np.split(freq, parts):
        angle = 2.0 * np.pi * (np.outer(cells, freqs) % length_z) / length_z
        rows.append(np.concatenate([np.cos(angle), -np.sin(angle)], 1))
    return np_halves(np.stack(rows))


def expand(source, out, back):
    size = source.shape[2]
    for part in range(2):
        for m in range(source.shape[1]):
            c = source[part, m, :, :size].astype(jnp.float32)
            s = source[part, m, :, size:].astype(jnp.float32)
            full = jnp.concatenate(
                [jnp.concatenate([c, s], axis=1), jnp.concatenate([-s, c], axis=1)], axis=0
            )
            out[part, m] = full.astype(jnp.bfloat16)
            back[part, m] = full.T.astype(jnp.bfloat16)


def whole_kernel(
    size_gx, size_gz, units,
    source_hbm, green_hbm, y_hbm, yback_hbm, x_hbm, z_hbm, out_ref,
    source, green, y_tab, y_back, x_half, z_half, x_tab, x_back, z_tab, z_back,
    raw_own, raw_other, green_own, green_sent, green_other, nyquist, distant,
    f_sent, f_got, b_sent, b_got, lines, spectrum, part_own, part_sent, part_other,
    local_sem, send_sem, raw_sem, green_sem, f_sem, b_sem, part_sem,
):
    gx, gy, gz = lax.axis_index("gx"), lax.axis_index("gy"), lax.axis_index("gz")
    blocks = size_gx * size_gz
    block = gx * size_gz + gz
    group = size_gz
    width = LANES // group
    rows = raw_own.shape[1]
    count_y = raw_own.shape[2]
    each = units // PARTS
    piece = 2 * each * rows
    share = green_own.shape[3]
    quarter = green_own.shape[2]
    half_x = 2 * quarter
    positions = 4 * units
    partner = {"gy": 1 - gy}
    lower = gy == 0
    packed = block + gy == 0

    def remote(source_at, target_at, sent, got, device):
        return pltpu.make_async_remote_copy(
            source_at, target_at, send_sem.at[sent], got,
            device_id=device, device_id_type=pl.DeviceIdType.MESH,
        )

    def plane_device(step):
        target = lax.rem(block + step, blocks)
        return target, {"gx": target // size_gz, "gz": lax.rem(target, size_gz)}

    def span(part, chunk, at):
        start = ((part * CHUNKS + chunk) * blocks + at) * piece
        return pl.ds(pl.multiple_of(start, 8), piece)

    def send_plane(sent_ref, got_ref, which, sems, part, chunk):
        def body(step, _):
            target, device = plane_device(step)
            remote(
                sent_ref.at[span(part, chunk, target), :],
                got_ref.at[span(part, chunk, block), :],
                which, sems.at[part, chunk], device,
            ).start()
            return 0

        lax.fori_loop(1, blocks, body, 0)
        got_ref[span(part, chunk, block), :] = sent_ref[span(part, chunk, block), :]

    def wait_plane(got_ref, which, sems, part, chunk):
        everything = got_ref.at[pl.ds(0, (blocks - 1) * piece), :]
        remote(everything, everything, which, sems.at[part, chunk], partner).wait_recv()

    step_x = rows * group
    copies = [
        pltpu.make_async_copy(
            source_hbm.at[pl.ds(c * step_x, step_x)], source.at[pl.ds(c * step_x, step_x)], local_sem.at[c]
        )
        for c in range(CHUNKS)
    ]
    copies += [
        pltpu.make_async_copy(green_hbm, green, local_sem.at[CHUNKS]),
        pltpu.make_async_copy(x_hbm, x_half, local_sem.at[CHUNKS + 1]),
        pltpu.make_async_copy(z_hbm, z_half, local_sem.at[CHUNKS + 2]),
        pltpu.make_async_copy(y_hbm.at[gy], y_tab, local_sem.at[CHUNKS + 3]),
        pltpu.make_async_copy(yback_hbm.at[gy], y_back, local_sem.at[CHUNKS + 4]),
    ]
    for copy in copies:
        copy.start()

    barrier = pltpu.get_barrier_semaphore()

    def greet(step, _):
        _, device = plane_device(step)
        pl.semaphore_signal(barrier, inc=1, device_id=device, device_id_type=pl.DeviceIdType.MESH)
        return 0

    pl.semaphore_signal(barrier, inc=1, device_id=partner, device_id_type=pl.DeviceIdType.MESH)
    lax.fori_loop(1, blocks, greet, 0)

    for c in range(CHUNKS):
        copies[c].wait()
        for a in range(rows):
            at = (c * rows + a) * group
            raw_own[c, a] = jnp.concatenate([source[at + b] for b in range(group)], axis=0).T

    pl.semaphore_wait(barrier, blocks)

    for c in range(CHUNKS):
        for a in range(rows):
            remote(raw_own.at[c, a], raw_other.at[c, a], 0, raw_sem.at[c, a], partner).start()

    copies[CHUNKS].wait()

    def extract(step, _):
        u, m = step // 4, lax.rem(step, 4)
        for half, out in ((gy, green_own), (1 - gy, green_sent)):
            at = m * positions + 2 * (half * units + u)
            out[u, m] = green[pl.ds(at, quarter, stride=4 * positions), :]
        return 0

    lax.fori_loop(0, 4 * units, extract, 0)
    for m in range(4):
        nyquist[m] = green[pl.ds(m * positions + 1, quarter, stride=4 * positions), :]
    copies[CHUNKS + 1].wait()
    copies[CHUNKS + 2].wait()
    expand(x_half, x_tab, x_back)
    expand(z_half, z_tab, z_back)
    copies[CHUNKS + 3].wait()
    copies[CHUNKS + 4].wait()

    def transform(c):
        def body(a, _):
            remote(raw_own.at[c, a], raw_other.at[c, a], 0, raw_sem.at[c, a], partner).wait_recv()
            own, other = raw_own[c, a], raw_other[c, a]
            cells = jnp.concatenate([jnp.where(lower, own, other), jnp.where(lower, other, own)], axis=0)
            freqs = table_left(y_tab[0], y_tab[1], cells)
            count = blocks * 2 * each
            for part in range(PARTS):
                start = (part * CHUNKS + c) * blocks * piece + a
                f_sent[pl.ds(start, count, stride=rows), :] = freqs[part * count : (part + 1) * count]
            return 0

        lax.fori_loop(0, rows, body, 0)

    for c in range(CHUNKS):
        transform(c)
        send_plane(f_sent, f_got, 1, f_sem, 0, c)
    for part in range(1, PARTS):
        for c in range(CHUNKS):
            send_plane(f_sent, f_got, 1, f_sem, part, c)

    def green_copy(u):
        return remote(green_sent.at[u], green_other.at[u], 2, green_sem.at[u], partner)

    distant_copy = remote(nyquist, distant, 3, green_sem.at[units], partner)
    green_copy(0).start()

    @pl.when(block + (1 - gy) == 0)
    def _():
        distant_copy.start()

    for u in range(1, units):
        green_copy(u).start()

    def forward(r0, r1, i0, i1):
        mixes = [(r0 + r1, i0 + i1), (r0 + i1, i0 - r1), (r0 - r1, i0 - i1), (r0 - i1, i0 + r1)]
        out = []
        for m, (real, imag) in enumerate(mixes):
            o = table_left(x_tab[0, m], x_tab[1, m], jnp.concatenate([real, imag], axis=0))
            out.append(jnp.concatenate([o[:quarter], o[quarter:]], axis=1))
        out = jnp.concatenate(out, axis=0)
        return [table_right(out, z_tab[0, h], z_tab[1, h]) for h in (gy, 1 - gy)]

    def unit_step(u, _):
        part, c = u // each, lax.rem(u, each)
        here = jnp.logical_and(packed, u == 0)

        @pl.when(c == 0)
        def _():
            for chunk in range(CHUNKS):
                wait_plane(f_got, 1, f_sem, part, chunk)

        def place(chunk, at, q):
            start = ((part * CHUNKS + chunk) * blocks + at) * piece + (2 * c + q) * rows
            return pl.ds(pl.multiple_of(start, 8), rows)

        for x in range(size_gx):
            for chunk in range(CHUNKS):
                for q in range(2):
                    pieces = [f_got[place(chunk, x * size_gz + g, q), :] for g in range(size_gz)]
                    at = q * half_x + (x * CHUNKS + chunk) * step_x
                    for b, moved in enumerate(block_swap(pieces, width)):
                        lines[at + b * rows : at + (b + 1) * rows] = moved

        field = lines[...]
        r0, r1 = field[:quarter], field[quarter:half_x]
        i0, i1 = field[half_x : half_x + quarter], field[half_x + quarter :]
        freqs = forward(r0, r1, jnp.where(here, 0.0, i0), jnp.where(here, 0.0, i1))
        green_copy(u).wait_recv()
        for side, gains in enumerate((green_own, green_other)):
            gain = gains[u].reshape(4 * quarter, share)
            spectrum[side] = jnp.concatenate([gain, gain], axis=1) * freqs[side]

        @pl.when(here)
        def _():
            distant_copy.wait_recv()
            i0 = lines[half_x : half_x + quarter]
            i1 = lines[half_x + quarter : 2 * half_x]
            zero = jnp.zeros_like(i0)
            for side, freqs in enumerate(forward(zero, zero, i0, i1)):
                gain = (nyquist, distant)[side][...].reshape(4 * quarter, share)
                spectrum[side] += jnp.concatenate([gain, gain], axis=1) * freqs

        inverse = sum(
            table_right(spectrum[side], z_back[0, h], z_back[1, h]) for side, h in ((0, gy), (1, 1 - gy))
        )
        near_r = near_i = far_r = far_i = 0.0
        for m in range(4):
            out = inverse[m * quarter : (m + 1) * quarter]
            both = jnp.concatenate([out[:, :LANES], out[:, LANES:]], axis=0)
            o = table_left(x_back[0, m], x_back[1, m], both)
            real, imag = o[:quarter], o[quarter:]
            near_r, near_i = near_r + real, near_i + imag
            turn_r, turn_i = [(real, imag), (-imag, real), (-real, -imag), (imag, -real)][m]
            far_r, far_i = far_r + turn_r, far_i + turn_i
        lines[...] = jnp.concatenate([near_r, far_r, near_i, far_i], axis=0)

        for x in range(size_gx):
            for chunk in range(CHUNKS):
                for q in range(2):
                    at = q * half_x + (x * CHUNKS + chunk) * step_x
                    pieces = [lines[at + b * rows : at + (b + 1) * rows] for b in range(group)]
                    for g, moved in enumerate(block_swap(pieces, width)):
                        b_sent[place(chunk, x * size_gz + g, q), :] = moved

        @pl.when(c == each - 1)
        def _():
            for chunk in range(CHUNKS):
                send_plane(b_sent, b_got, 4, b_sem, part, chunk)

        return 0

    lax.fori_loop(0, units, unit_step, 0)

    def part_copy(c, a):
        return remote(part_sent.at[c, a], part_other.at[c, a], 5, part_sem.at[c, a], partner)

    def invert(c):
        for part in range(PARTS):
            wait_plane(b_got, 4, b_sem, part, c)

        def body(a, _):
            count = blocks * 2 * each
            freqs = jnp.concatenate(
                [
                    b_got[pl.ds((part * CHUNKS + c) * blocks * piece + a, count, stride=rows), :]
                    for part in range(PARTS)
                ],
                axis=0,
            )
            cells = table_left(y_back[0], y_back[1], freqs)
            low, high = cells[:count_y], cells[count_y:]
            part_sent[c, a] = jnp.where(lower, high, low)
            part_own[c, a] = jnp.where(lower, low, high)
            part_copy(c, a).start()
            return 0

        lax.fori_loop(0, rows, body, 0)

    for c in range(CHUNKS):
        invert(c)

    for c in range(CHUNKS):
        def finish(a, _):
            part_copy(c, a).wait_recv()
            out_ref[c * rows + a] = part_own[c, a] + part_other[c, a]
            return 0

        lax.fori_loop(0, rows, finish, 0)

    remote(raw_own, raw_other, 0, raw_sem.at[0, 0], partner).wait_send()
    moved = f_sent.at[pl.ds(0, PARTS * CHUNKS * (blocks - 1) * piece), :]
    remote(moved, moved, 1, f_sem.at[0, 0], partner).wait_send()
    remote(green_sent, green_other, 2, green_sem.at[0], partner).wait_send()

    @pl.when(block + (1 - gy) == 0)
    def _():
        distant_copy.wait_send()

    remote(moved, moved, 4, b_sem.at[0, 0], partner).wait_send()
    remote(part_sent, part_other, 5, part_sem.at[0, 0], partner).wait_send()


def unpack_kernel(in_ref, out_ref):
    width = out_ref.shape[1]
    group = LANES // width
    for row in range(in_ref.shape[0]):
        block = in_ref[row].T
        for b in range(group):
            out_ref[row * group + b] = block[b * width : (b + 1) * width]


def f32(*shape):
    return jax.ShapeDtypeStruct(shape, jnp.float32)


def fast_device(source, green):
    size_gx = lax.axis_size("gx")
    size_gy = lax.axis_size("gy")
    size_gz = lax.axis_size("gz")
    brick_x, brick_y, brick_z = source.shape
    long_x, places, share = green.shape
    long_y = 2 * brick_y * size_gy
    long_z = 2 * brick_z * size_gz
    blocks = size_gx * size_gz
    units = places // (2 * size_gy)
    group = LANES // brick_z
    rows = brick_x // group // CHUNKS
    quarter = long_x // 4
    y_tab, y_back = y_tables(long_y, blocks, units, 1.0 / (long_x * long_z))
    x_tab, z_tab = x_table(long_x, group, rows), z_table(long_z, 2)
    lines = blocks * units * 2 * CHUNKS * rows
    vmem = lambda *shape: pltpu.VMEM(shape, jnp.float32)
    half = lambda *shape: pltpu.VMEM(shape, jnp.bfloat16)
    raw = (CHUNKS, rows, brick_y, LANES)
    slots = (units, 4, quarter, share)
    parts = pl.pallas_call(
        functools.partial(whole_kernel, size_gx, size_gz, units),
        out_shape=f32(CHUNKS * rows, brick_y, LANES),
        in_specs=[pl.BlockSpec(memory_space=pltpu.HBM)] * 6,
        out_specs=pl.BlockSpec(memory_space=pltpu.VMEM),
        scratch_shapes=[
            vmem(brick_x, brick_z, brick_y),
            vmem(long_x * places, share),
            half(*y_tab.shape[1:]),
            half(*y_back.shape[1:]),
            half(*x_tab.shape),
            half(*z_tab.shape),
            half(2, 4, 2 * quarter, 2 * quarter),
            half(2, 4, 2 * quarter, 2 * quarter),
            half(2, 2, long_z, 2 * share),
            half(2, 2, long_z, 2 * share),
            vmem(*raw),
            vmem(*raw),
            vmem(*slots),
            vmem(*slots),
            vmem(*slots),
            vmem(*slots[1:]),
            vmem(*slots[1:]),
            vmem(lines, LANES),
            vmem(lines, LANES),
            vmem(lines, LANES),
            vmem(lines, LANES),
            vmem(long_x, LANES),
            vmem(2, long_x, 2 * share),
            vmem(*raw),
            vmem(*raw),
            vmem(*raw),
            pltpu.SemaphoreType.DMA((CHUNKS + 5,)),
            pltpu.SemaphoreType.DMA((6,)),
            pltpu.SemaphoreType.DMA((CHUNKS, rows)),
            pltpu.SemaphoreType.DMA((units + 1,)),
            pltpu.SemaphoreType.DMA((PARTS, CHUNKS)),
            pltpu.SemaphoreType.DMA((PARTS, CHUNKS)),
            pltpu.SemaphoreType.DMA((CHUNKS, rows)),
        ],
        compiler_params=pltpu.CompilerParams(
            vmem_limit_bytes=VMEM_BYTES, collective_id=0, has_side_effects=True
        ),
    )(jnp.swapaxes(source, 1, 2), green.reshape(long_x * places, share), y_tab, y_back, x_tab, z_tab)
    result = pl.pallas_call(
        unpack_kernel,
        out_shape=f32(brick_x, brick_z, brick_y),
        compiler_params=pltpu.CompilerParams(vmem_limit_bytes=VMEM_BYTES),
    )(parts)
    return jnp.swapaxes(result, 1, 2)


def fits(sizes, source, green):
    brick_x, brick_y, brick_z = source.shape
    units = green.shape[1] // (2 * sizes["gy"])
    return (
        brick_z * sizes["gz"] == LANES
        and green.shape[2] == LANES
        and sizes["gx"] * brick_x == 2 * LANES
        and brick_y * sizes["gy"] == LANES
        and brick_x * brick_z == 8 * CHUNKS * LANES
        and units % PARTS == 0
        and sizes["gy"] == 2
    )


def phase_table(row_index, column_index, length):
    phase_index = row_index[:, None] * column_index[None, :] % length
    angles = phase_index.astype(jnp.float32) * (2.0 * math.pi / length)
    return (jnp.cos(angles), jnp.sin(angles))


def pair_frequency(position, length):
    unit_index = position // 2
    member = position % 2
    return jnp.where(
        unit_index == 0,
        member * (length // 2),
        jnp.where(member == 0, unit_index, length - unit_index),
    )


def product(form, left, table):
    return jnp.einsum(form, left, table, precision=lax.Precision.HIGHEST)


def mirror_plane(field, first_block):
    flipped = jnp.roll(jnp.flip(field, 1), 1, 1)
    count_y, count_x = field.shape
    swapped = flipped.reshape(count_y // 2, 2, count_x)[:, ::-1, :].reshape(count_y, count_x)
    local_row = lax.iota(jnp.int32, count_y)
    keep_unit = jnp.logical_and(first_block, local_row < 2)
    return jnp.where(keep_unit[:, None], flipped, swapped)


def per_device(source, green):
    size_gx = lax.axis_size("gx")
    size_gy = lax.axis_size("gy")
    size_gz = lax.axis_size("gz")
    brick_x, brick_y, brick_z = source.shape
    if fits({"gx": size_gx, "gy": size_gy, "gz": size_gz}, source, green):
        return fast_device(source, green)
    grid_x = brick_x * size_gx
    grid_y = brick_y * size_gy
    grid_z = brick_z * size_gz
    long_x = 2 * grid_x
    long_y = 2 * grid_y
    long_z = 2 * grid_z
    cell_z = lax.iota(jnp.int32, grid_z)
    parity_sign = (1 - 2 * (cell_z % 2)).astype(jnp.float32)
    z_lines = lax.all_to_all(source, "gz", split_axis=0, concat_axis=2, tiled=True)
    kept_freq = lax.iota(jnp.int32, long_z // 2)
    z_cos, z_sin = phase_table(cell_z, kept_freq, long_z)
    z_sin = jnp.where(kept_freq[None, :] == 0, -parity_sign[:, None], z_sin)
    z_real = product("abn,nk->abk", z_lines, z_cos)
    z_imag = -product("abn,nk->abk", z_lines, z_sin)
    y_real, y_imag = (
        lax.all_to_all(z_real, "gy", split_axis=2, concat_axis=1, tiled=True),
        lax.all_to_all(z_imag, "gy", split_axis=2, concat_axis=1, tiled=True),
    )
    y_cos, y_sin = phase_table(
        lax.iota(jnp.int32, grid_y), pair_frequency(lax.iota(jnp.int32, long_y), long_y), long_y
    )
    fy_real = product("ayc,yk->ack", y_real, y_cos) + product("ayc,yk->ack", y_imag, y_sin)
    fy_imag = product("ayc,yk->ack", y_imag, y_cos) - product("ayc,yk->ack", y_real, y_sin)
    x_real, x_imag = (
        lax.all_to_all(fy_real, ("gx", "gz"), split_axis=2, concat_axis=0, tiled=True),
        lax.all_to_all(fy_imag, ("gx", "gz"), split_axis=2, concat_axis=0, tiled=True),
    )
    x_rows = lax.iota(jnp.int32, grid_x)
    x_cos, x_sin = phase_table(x_rows, lax.iota(jnp.int32, long_x), long_x)
    full_real = product("xck,xj->ckj", x_real, x_cos) + product("xck,xj->ckj", x_imag, x_sin)
    full_imag = product("xck,xj->ckj", x_imag, x_cos) - product("xck,xj->ckj", x_real, x_sin)
    kept_green = jnp.transpose(green[:, :, 0::2], (2, 1, 0))
    nyquist_green = jnp.transpose(green[:, :, 1], (1, 0))
    prod_real = kept_green * full_real
    prod_imag = kept_green * full_imag
    first_block = lax.axis_index("gx") * size_gz + lax.axis_index("gz") == 0
    first_slab = lax.axis_index("gy") == 0
    base_real = full_real[0]
    base_imag = full_imag[0]
    mirror_real = mirror_plane(base_real, first_block)
    mirror_imag = mirror_plane(base_imag, first_block)
    zero_real = 0.5 * (base_real + mirror_real)
    zero_imag = 0.5 * (base_imag - mirror_imag)
    nyq_real = 0.5 * (base_imag + mirror_imag)
    nyq_imag = 0.5 * (mirror_real - base_real)
    zero_green = kept_green[0]
    packed_real = zero_green * zero_real - nyquist_green * nyq_imag
    packed_imag = zero_green * zero_imag + nyquist_green * nyq_real
    slot_mask = jnp.logical_and(lax.iota(jnp.int32, prod_real.shape[0]) == 0, first_slab)
    prod_real = jnp.where(slot_mask[:, None, None], packed_real[None], prod_real)
    prod_imag = jnp.where(slot_mask[:, None, None], packed_imag[None], prod_imag)
    inv_xcos, inv_xsin = phase_table(
        lax.iota(jnp.int32, long_x), lax.iota(jnp.int32, grid_x), long_x
    )
    back_real = (
        product("ckj,jx->ckx", prod_real, inv_xcos) - product("ckj,jx->ckx", prod_imag, inv_xsin)
    ) / long_x
    back_imag = (
        product("ckj,jx->ckx", prod_imag, inv_xcos) + product("ckj,jx->ckx", prod_real, inv_xsin)
    ) / long_x
    mid_real, mid_imag = (
        lax.all_to_all(back_real, ("gx", "gz"), split_axis=2, concat_axis=1, tiled=True),
        lax.all_to_all(back_imag, ("gx", "gz"), split_axis=2, concat_axis=1, tiled=True),
    )
    y_order = lax.iota(jnp.int32, long_y)
    inv_ycos, inv_ysin = phase_table(
        pair_frequency(y_order, long_y), lax.iota(jnp.int32, grid_y), long_y
    )
    half_real = (
        product("cja,jy->cay", mid_real, inv_ycos) - product("cja,jy->cay", mid_imag, inv_ysin)
    ) / long_y
    half_imag = (
        product("cja,jy->cay", mid_imag, inv_ycos) + product("cja,jy->cay", mid_real, inv_ysin)
    ) / long_y
    last_real, last_imag = (
        lax.all_to_all(half_real, "gy", split_axis=2, concat_axis=0, tiled=True),
        lax.all_to_all(half_imag, "gy", split_axis=2, concat_axis=0, tiled=True),
    )
    kept_freq = lax.iota(jnp.int32, long_z // 2)
    base_cos, base_sin = phase_table(kept_freq, cell_z, long_z)
    inv_zcos = jnp.where(kept_freq[:, None] == 0, 1.0, 2.0 * base_cos)
    inv_zsin = jnp.where(kept_freq[:, None] == 0, -parity_sign[None, :], 2.0 * base_sin)
    result = (
        product("jab,jn->abn", last_real, inv_zcos) - product("jab,jn->abn", last_imag, inv_zsin)
    ) / long_z
    return lax.all_to_all(result, "gz", split_axis=2, concat_axis=0, tiled=True)


def solution(mesh):
    step = jax.shard_map(
        per_device,
        mesh=mesh,
        in_specs=(P("gx", "gy", "gz"), P(None, ("gx", "gz"), "gy")),
        out_specs=P("gx", "gy", "gz"),
        check_vma=False,
    )
    return step
```

```python
import functools
import math

import jax
import jax.numpy as jnp
import ml_dtypes
import numpy as np
from jax import lax
from jax.experimental import pallas as pl
from jax.experimental.pallas import tpu as pltpu
from jax.sharding import PartitionSpec as P

LANES = 128
PARTS = 2
CHUNKS = 4
VMEM_BYTES = 63 * 1024 * 1024


def np_halves(table):
    high = table.astype(np.float32).astype(ml_dtypes.bfloat16)
    low = (table - high.astype(np.float64)).astype(np.float32).astype(ml_dtypes.bfloat16)
    return np.stack([high, low])


def split(value):
    high = value.astype(jnp.bfloat16)
    return high, (value - high.astype(jnp.float32)).astype(jnp.bfloat16)


def mm(left, right):
    return jnp.dot(left, right, preferred_element_type=jnp.float32)


def table_left(high, low, value):
    v_high, v_low = split(value)
    both = mm(high, jnp.concatenate([v_high, v_low], axis=1))
    width = value.shape[1]
    return both[:, :width] + (both[:, width:] + mm(low, v_high))


def table_right(value, high, low):
    v_high, v_low = split(value)
    return mm(v_high, high) + (mm(v_low, high) + mm(v_high, low))


def block_swap(pieces, width):
    count = len(pieces)
    group = lax.broadcasted_iota(jnp.int32, pieces[0].shape, 1) // width
    out = []
    for c in range(count):
        total = None
        for g in range(count):
            moved = pieces[g]
            shift = (g - c) * width % LANES
            if shift:
                moved = pltpu.roll(moved, shift, 1)
            total = moved if total is None else jnp.where(group == g, moved, total)
        out.append(total)
    return out


def y_tables(length_y, blocks, units, scale):
    cells = np.arange(length_y // 2)
    freq = np.arange(length_y // 2)
    angle = 2.0 * np.pi * (np.outer(freq, cells) % length_y) / length_y
    sign = 1.0 - 2.0 * (cells % 2)
    real, imag = np.cos(angle), -np.sin(angle)
    imag[0] = sign
    weight = np.where(freq == 0, 1.0, 2.0)[:, None] * (scale / length_y)
    both = np.stack([real, imag], axis=1)
    back = both * weight[:, None]

    def ordered(table):
        table = table.reshape(blocks, 2, PARTS, units // PARTS, 2, -1)
        return table.transpose(1, 2, 0, 3, 4, 5).reshape(2, length_y // 2, -1)

    forward = np.swapaxes(np_halves(ordered(both)), 0, 1)
    backward = np.swapaxes(np_halves(np.swapaxes(ordered(back), 1, 2)), 0, 1)
    return forward, backward


def x_table(length_x, group, rows):
    freqs = np.arange(length_x // 4)[:, None]
    place = np.arange(length_x // 2)[None, :]
    a, q = place % rows, place // rows % 2
    b, block = place // (2 * rows) % group, place // (2 * rows * group)
    cells = (block * rows + a) * group + b
    out = []
    for member in range(4):
        angle = 2.0 * np.pi * ((4 * freqs + member) * cells % length_x) / length_x
        c, s = np.cos(angle), np.sin(angle)
        out.append(np.concatenate([np.where(q == 0, c, s), np.where(q == 0, -s, c)], 0))
    return np_halves(np.stack(out))


def z_table(length_z, parts):
    place = np.arange(length_z)
    unit, member = place // 2, place % 2
    freq = np.where(unit == 0, member * (length_z // 2), np.where(member == 0, unit, length_z - unit))
    cells = np.arange(length_z // 2)
    rows = []
    for freqs in np.split(freq, parts):
        angle = 2.0 * np.pi * (np.outer(cells, freqs) % length_z) / length_z
        rows.append(np.concatenate([np.cos(angle), -np.sin(angle)], 1))
    return np_halves(np.stack(rows))


def expand(source, out, back):
    size = source.shape[1] // 2
    for at in range(source.shape[0] // size):
        c = source[at * size : (at + 1) * size, :size].astype(jnp.float32)
        s = source[at * size : (at + 1) * size, size:].astype(jnp.float32)
        full = jnp.concatenate(
            [jnp.concatenate([c, s], axis=1), jnp.concatenate([-s, c], axis=1)], axis=0
        )
        out[at] = full.astype(jnp.bfloat16)
        back[at] = full.T.astype(jnp.bfloat16)


def transposed(source, back):
    size = source.shape[1]
    for at in range(source.shape[0] // size):
        block = source[at * size : (at + 1) * size, :]
        back[at] = block.astype(jnp.float32).T.astype(jnp.bfloat16)


def whole_kernel(
    size_gx, size_gz, units,
    source_hbm, green_hbm, tables_hbm, out_ref,
    source, green, y_both, x_tab, x_back, z_half, z_tab, z_back,
    raw_own, raw_other, green_own, green_sent, green_other, nyquist, distant,
    f_sent, f_got, b_sent, b_got, lines, spectrum, part_own, part_sent, part_other,
    local_sem, send_sem, raw_sem, green_sem, f_sem, b_sem, part_sem,
):
    gx, gy, gz = lax.axis_index("gx"), lax.axis_index("gy"), lax.axis_index("gz")
    blocks = size_gx * size_gz
    block = gx * size_gz + gz
    group = size_gz
    width = LANES // group
    rows = raw_own.shape[1]
    count_y = raw_own.shape[2]
    lines_y = 2 * count_y
    each = units // PARTS
    piece = 2 * each * rows
    share = green_own.shape[3]
    quarter = green_own.shape[2]
    half_x = 2 * quarter
    positions = 4 * units
    partner = {"gy": 1 - gy}
    lower = gy == 0
    packed = block + gy == 0

    def remote(source_at, target_at, sent, got, device):
        return pltpu.make_async_remote_copy(
            source_at, target_at, send_sem.at[sent], got,
            device_id=device, device_id_type=pl.DeviceIdType.MESH,
        )

    def plane_device(step):
        target = lax.rem(block + step, blocks)
        return target, {"gx": target // size_gz, "gz": lax.rem(target, size_gz)}

    def span(part, chunk, at):
        start = ((part * CHUNKS + chunk) * blocks + at) * piece
        return pl.ds(pl.multiple_of(start, 8), piece)

    def send_plane(sent_ref, got_ref, which, sems, part, chunk):
        def body(step, _):
            target, device = plane_device(step)
            remote(
                sent_ref.at[span(part, chunk, target), :],
                got_ref.at[span(part, chunk, block), :],
                which, sems.at[part, chunk], device,
            ).start()
            return 0

        lax.fori_loop(1, blocks, body, 0)
        got_ref[span(part, chunk, block), :] = sent_ref[span(part, chunk, block), :]

    def wait_plane(got_ref, which, sems, part, chunk):
        everything = got_ref.at[pl.ds(0, (blocks - 1) * piece), :]
        remote(everything, everything, which, sems.at[part, chunk], partner).wait_recv()

    step_x = rows * group
    copies = [
        pltpu.make_async_copy(
            source_hbm.at[pl.ds(c * step_x, step_x)], source.at[pl.ds(c * step_x, step_x)], local_sem.at[c]
        )
        for c in range(CHUNKS)
    ]
    copies.append(pltpu.make_async_copy(green_hbm, green, local_sem.at[CHUNKS]))
    start = 0
    for n, (table, which) in enumerate(((x_tab, None), (z_half, None), (y_both, gy))):
        size = table.shape[0]
        at = start if which is None else start + which * size
        copies.append(
            pltpu.make_async_copy(
                tables_hbm.at[pl.ds(at, size), :], table, local_sem.at[CHUNKS + 1 + n]
            )
        )
        start += size
    for copy in copies:
        copy.start()

    barrier = pltpu.get_barrier_semaphore()

    def greet(step, _):
        _, device = plane_device(step)
        pl.semaphore_signal(barrier, inc=1, device_id=device, device_id_type=pl.DeviceIdType.MESH)
        return 0

    pl.semaphore_signal(barrier, inc=1, device_id=partner, device_id_type=pl.DeviceIdType.MESH)
    lax.fori_loop(1, blocks, greet, 0)

    for c in range(CHUNKS):
        copies[c].wait()
        for a in range(rows):
            at = (c * rows + a) * group
            raw_own[c, a] = jnp.concatenate([source[at + b] for b in range(group)], axis=0).T

    pl.semaphore_wait(barrier, blocks)

    for c in range(CHUNKS):
        for a in range(rows):
            remote(raw_own.at[c, a], raw_other.at[c, a], 0, raw_sem.at[c, a], partner).start()

    copies[CHUNKS].wait()

    def extract(step, _):
        u, m = step // 4, lax.rem(step, 4)
        for half, out in ((gy, green_own), (1 - gy, green_sent)):
            at = m * positions + 2 * (half * units + u)
            out[u, m] = green[pl.ds(at, quarter, stride=4 * positions), :]
        return 0

    lax.fori_loop(0, 4 * units, extract, 0)
    for m in range(4):
        nyquist[m] = green[pl.ds(m * positions + 1, quarter, stride=4 * positions), :]
    copies[CHUNKS + 1].wait()
    transposed(x_tab, x_back)
    copies[CHUNKS + 2].wait()
    expand(z_half, z_tab, z_back)
    copies[CHUNKS + 3].wait()

    def transform(c):
        def body(a, _):
            remote(raw_own.at[c, a], raw_other.at[c, a], 0, raw_sem.at[c, a], partner).wait_recv()
            own, other = raw_own[c, a], raw_other[c, a]
            cells = jnp.concatenate([jnp.where(lower, own, other), jnp.where(lower, other, own)], axis=0)
            freqs = table_left(y_both[:lines_y, :lines_y], y_both[lines_y:, :lines_y], cells)
            count = blocks * 2 * each
            for part in range(PARTS):
                start = (part * CHUNKS + c) * blocks * piece + a
                f_sent[pl.ds(start, count, stride=rows), :] = freqs[part * count : (part + 1) * count]
            return 0

        lax.fori_loop(0, rows, body, 0)

    for c in range(CHUNKS):
        transform(c)
        send_plane(f_sent, f_got, 1, f_sem, 0, c)
    for part in range(1, PARTS):
        for c in range(CHUNKS):
            send_plane(f_sent, f_got, 1, f_sem, part, c)

    def green_copy(u):
        return remote(green_sent.at[u], green_other.at[u], 2, green_sem.at[u], partner)

    distant_copy = remote(nyquist, distant, 3, green_sem.at[units], partner)
    green_copy(0).start()

    @pl.when(block + (1 - gy) == 0)
    def _():
        distant_copy.start()

    for u in range(1, units):
        green_copy(u).start()

    def turned(value):
        tiles = value.reshape(-1, 2 * rows, LANES)
        real = lax.broadcasted_iota(jnp.int32, tiles.shape, 1) < rows
        moved = pltpu.roll(tiles, rows, 1)
        return jnp.where(real, moved, -moved).reshape(value.shape)

    def forward(field):
        near, far = field[:half_x], field[half_x:]
        twist = turned(far)
        out = []
        for m, cells in enumerate((near + far, near + twist, near - far, near - twist)):
            high, low = (x_tab[(4 * part + m) * half_x : (4 * part + m + 1) * half_x, :] for part in range(2))
            o = table_left(high, low, cells)
            out.append(jnp.concatenate([o[:quarter], o[quarter:]], axis=1))
        out = jnp.concatenate(out, axis=0)
        return [table_right(out, z_tab[h], z_tab[2 + h]) for h in (gy, 1 - gy)]

    def unit_step(u, _):
        part, c = u // each, lax.rem(u, each)
        here = jnp.logical_and(packed, u == 0)

        @pl.when(c == 0)
        def _():
            for chunk in range(CHUNKS):
                wait_plane(f_got, 1, f_sem, part, chunk)

        def place(chunk, at):
            start = ((part * CHUNKS + chunk) * blocks + at) * piece + 2 * c * rows
            return pl.ds(pl.multiple_of(start, 8), 2 * rows)

        for x in range(size_gx):
            for chunk in range(CHUNKS):
                pieces = [f_got[place(chunk, x * size_gz + g), :] for g in range(size_gz)]
                at = (x * CHUNKS + chunk) * 2 * step_x
                for b, moved in enumerate(block_swap(pieces, width)):
                    lines[at + 2 * b * rows : at + 2 * (b + 1) * rows] = moved

        def masked(keep_real):
            field = lines[...]
            tiles = field.reshape(-1, 2 * rows, LANES)
            real = lax.broadcasted_iota(jnp.int32, tiles.shape, 1) < rows
            keep = jnp.logical_or(real == keep_real, jnp.logical_not(here))
            return jnp.where(keep, tiles, 0.0).reshape(field.shape)

        freqs = forward(masked(True))
        green_copy(u).wait_recv()
        for side, gains in enumerate((green_own, green_other)):
            gain = gains[u].reshape(4 * quarter, share)
            spectrum[side] = jnp.concatenate([gain, gain], axis=1) * freqs[side]

        @pl.when(here)
        def _():
            distant_copy.wait_recv()
            for side, freqs in enumerate(forward(masked(False))):
                gain = (nyquist, distant)[side][...].reshape(4 * quarter, share)
                spectrum[side] += jnp.concatenate([gain, gain], axis=1) * freqs

        inverse = sum(
            table_right(spectrum[side], z_back[h], z_back[2 + h]) for side, h in ((0, gy), (1, 1 - gy))
        )
        cells = []
        for m in range(4):
            out = inverse[m * quarter : (m + 1) * quarter]
            both = jnp.concatenate([out[:, :LANES], out[:, LANES:]], axis=0)
            cells.append(table_left(x_back[m], x_back[4 + m], both))
        even, odd = cells[0] + cells[2], cells[1] + cells[3]
        lines[:half_x] = even + odd
        lines[half_x:] = (cells[0] - cells[2]) - turned(cells[1] - cells[3])

        for x in range(size_gx):
            for chunk in range(CHUNKS):
                at = (x * CHUNKS + chunk) * 2 * step_x
                pieces = [lines[at + 2 * b * rows : at + 2 * (b + 1) * rows] for b in range(group)]
                for g, moved in enumerate(block_swap(pieces, width)):
                    b_sent[place(chunk, x * size_gz + g), :] = moved

        @pl.when(c == each - 1)
        def _():
            for chunk in range(CHUNKS):
                send_plane(b_sent, b_got, 4, b_sem, part, chunk)

        return 0

    lax.fori_loop(0, units, unit_step, 0)

    def part_copy(c, a):
        return remote(part_sent.at[c, a], part_other.at[c, a], 5, part_sem.at[c, a], partner)

    def invert(c):
        for part in range(PARTS):
            wait_plane(b_got, 4, b_sem, part, c)

        def body(a, _):
            count = blocks * 2 * each
            freqs = jnp.concatenate(
                [
                    b_got[pl.ds((part * CHUNKS + c) * blocks * piece + a, count, stride=rows), :]
                    for part in range(PARTS)
                ],
                axis=0,
            )
            cells = table_left(y_both[:lines_y, lines_y:], y_both[lines_y:, lines_y:], freqs)
            low, high = cells[:count_y], cells[count_y:]
            part_sent[c, a] = jnp.where(lower, high, low)
            part_own[c, a] = jnp.where(lower, low, high)
            part_copy(c, a).start()
            return 0

        lax.fori_loop(0, rows, body, 0)

    for c in range(CHUNKS):
        invert(c)

    for c in range(CHUNKS):
        def finish(a, _):
            part_copy(c, a).wait_recv()
            out_ref[c * rows + a] = part_own[c, a] + part_other[c, a]
            return 0

        lax.fori_loop(0, rows, finish, 0)

    remote(raw_own, raw_other, 0, raw_sem.at[0, 0], partner).wait_send()
    moved = f_sent.at[pl.ds(0, PARTS * CHUNKS * (blocks - 1) * piece), :]
    remote(moved, moved, 1, f_sem.at[0, 0], partner).wait_send()
    remote(green_sent, green_other, 2, green_sem.at[0], partner).wait_send()

    @pl.when(block + (1 - gy) == 0)
    def _():
        distant_copy.wait_send()

    remote(moved, moved, 4, b_sem.at[0, 0], partner).wait_send()
    remote(part_sent, part_other, 5, part_sem.at[0, 0], partner).wait_send()


def unpack_kernel(in_ref, out_ref):
    width = out_ref.shape[1]
    group = LANES // width
    for row in range(in_ref.shape[0]):
        block = in_ref[row].T
        for b in range(group):
            out_ref[row * group + b] = block[b * width : (b + 1) * width]


def f32(*shape):
    return jax.ShapeDtypeStruct(shape, jnp.float32)


def fast_device(source, green):
    size_gx = lax.axis_size("gx")
    size_gy = lax.axis_size("gy")
    size_gz = lax.axis_size("gz")
    brick_x, brick_y, brick_z = source.shape
    long_x, places, share = green.shape
    long_y = 2 * brick_y * size_gy
    long_z = 2 * brick_z * size_gz
    blocks = size_gx * size_gz
    units = places // (2 * size_gy)
    group = LANES // brick_z
    rows = brick_x // group // CHUNKS
    quarter = long_x // 4
    y_tab, y_back = y_tables(long_y, blocks, units, 1.0 / (long_x * long_z))
    x_tab, z_tab = x_table(long_x, group, rows), z_table(long_z, 2)
    flat = lambda table: table.reshape(-1, 2 * share)
    y_both = np.concatenate([y_tab, y_back], axis=3)
    tables = np.concatenate([flat(x_tab), flat(z_tab), flat(y_both)])
    lines = blocks * units * 2 * CHUNKS * rows
    vmem = lambda *shape: pltpu.VMEM(shape, jnp.float32)
    half = lambda *shape: pltpu.VMEM(shape, jnp.bfloat16)
    raw = (CHUNKS, rows, brick_y, LANES)
    slots = (units, 4, quarter, share)
    parts = pl.pallas_call(
        functools.partial(whole_kernel, size_gx, size_gz, units),
        out_shape=f32(CHUNKS * rows, brick_y, LANES),
        in_specs=[pl.BlockSpec(memory_space=pltpu.HBM)] * 3,
        out_specs=pl.BlockSpec(memory_space=pltpu.VMEM),
        scratch_shapes=[
            vmem(brick_x, brick_z, brick_y),
            vmem(long_x * places, share),
            half(*flat(y_both[0]).shape),
            half(*flat(x_tab).shape),
            half(8, 2 * quarter, 2 * quarter),
            half(*flat(z_tab).shape),
            half(4, long_z, 2 * share),
            half(4, long_z, 2 * share),
            vmem(*raw),
            vmem(*raw),
            vmem(*slots),
            vmem(*slots),
            vmem(*slots),
            vmem(*slots[1:]),
            vmem(*slots[1:]),
            vmem(lines, LANES),
            vmem(lines, LANES),
            vmem(lines, LANES),
            vmem(lines, LANES),
            vmem(long_x, LANES),
            vmem(2, long_x, 2 * share),
            vmem(*raw),
            vmem(*raw),
            vmem(*raw),
            pltpu.SemaphoreType.DMA((CHUNKS + 4,)),
            pltpu.SemaphoreType.DMA((6,)),
            pltpu.SemaphoreType.DMA((CHUNKS, rows)),
            pltpu.SemaphoreType.DMA((units + 1,)),
            pltpu.SemaphoreType.DMA((PARTS, CHUNKS)),
            pltpu.SemaphoreType.DMA((PARTS, CHUNKS)),
            pltpu.SemaphoreType.DMA((CHUNKS, rows)),
        ],
        compiler_params=pltpu.CompilerParams(
            vmem_limit_bytes=VMEM_BYTES, collective_id=0, has_side_effects=True
        ),
    )(jnp.swapaxes(source, 1, 2), green.reshape(long_x * places, share), tables)
    result = pl.pallas_call(
        unpack_kernel,
        out_shape=f32(brick_x, brick_z, brick_y),
        compiler_params=pltpu.CompilerParams(vmem_limit_bytes=VMEM_BYTES),
    )(parts)
    return jnp.swapaxes(result, 1, 2)


def fits(sizes, source, green):
    brick_x, brick_y, brick_z = source.shape
    units = green.shape[1] // (2 * sizes["gy"])
    return (
        brick_z * sizes["gz"] == LANES
        and green.shape[2] == LANES
        and sizes["gx"] * brick_x == 2 * LANES
        and brick_y * sizes["gy"] == LANES
        and brick_x * brick_z == 4 * CHUNKS * LANES
        and units % PARTS == 0
        and sizes["gy"] == 2
    )


def phase_table(row_index, column_index, length):
    phase_index = row_index[:, None] * column_index[None, :] % length
    angles = phase_index.astype(jnp.float32) * (2.0 * math.pi / length)
    return (jnp.cos(angles), jnp.sin(angles))


def pair_frequency(position, length):
    unit_index = position // 2
    member = position % 2
    return jnp.where(
        unit_index == 0,
        member * (length // 2),
        jnp.where(member == 0, unit_index, length - unit_index),
    )


def product(form, left, table):
    return jnp.einsum(form, left, table, precision=lax.Precision.HIGHEST)


def mirror_plane(field, first_block):
    flipped = jnp.roll(jnp.flip(field, 1), 1, 1)
    count_y, count_x = field.shape
    swapped = flipped.reshape(count_y // 2, 2, count_x)[:, ::-1, :].reshape(count_y, count_x)
    local_row = lax.iota(jnp.int32, count_y)
    keep_unit = jnp.logical_and(first_block, local_row < 2)
    return jnp.where(keep_unit[:, None], flipped, swapped)


def per_device(source, green):
    size_gx = lax.axis_size("gx")
    size_gy = lax.axis_size("gy")
    size_gz = lax.axis_size("gz")
    brick_x, brick_y, brick_z = source.shape
    if fits({"gx": size_gx, "gy": size_gy, "gz": size_gz}, source, green):
        return fast_device(source, green)
    grid_x = brick_x * size_gx
    grid_y = brick_y * size_gy
    grid_z = brick_z * size_gz
    long_x = 2 * grid_x
    long_y = 2 * grid_y
    long_z = 2 * grid_z
    cell_z = lax.iota(jnp.int32, grid_z)
    parity_sign = (1 - 2 * (cell_z % 2)).astype(jnp.float32)
    z_lines = lax.all_to_all(source, "gz", split_axis=0, concat_axis=2, tiled=True)
    kept_freq = lax.iota(jnp.int32, long_z // 2)
    z_cos, z_sin = phase_table(cell_z, kept_freq, long_z)
    z_sin = jnp.where(kept_freq[None, :] == 0, -parity_sign[:, None], z_sin)
    z_real = product("abn,nk->abk", z_lines, z_cos)
    z_imag = -product("abn,nk->abk", z_lines, z_sin)
    y_real, y_imag = (
        lax.all_to_all(z_real, "gy", split_axis=2, concat_axis=1, tiled=True),
        lax.all_to_all(z_imag, "gy", split_axis=2, concat_axis=1, tiled=True),
    )
    y_cos, y_sin = phase_table(
        lax.iota(jnp.int32, grid_y), pair_frequency(lax.iota(jnp.int32, long_y), long_y), long_y
    )
    fy_real = product("ayc,yk->ack", y_real, y_cos) + product("ayc,yk->ack", y_imag, y_sin)
    fy_imag = product("ayc,yk->ack", y_imag, y_cos) - product("ayc,yk->ack", y_real, y_sin)
    x_real, x_imag = (
        lax.all_to_all(fy_real, ("gx", "gz"), split_axis=2, concat_axis=0, tiled=True),
        lax.all_to_all(fy_imag, ("gx", "gz"), split_axis=2, concat_axis=0, tiled=True),
    )
    x_rows = lax.iota(jnp.int32, grid_x)
    x_cos, x_sin = phase_table(x_rows, lax.iota(jnp.int32, long_x), long_x)
    full_real = product("xck,xj->ckj", x_real, x_cos) + product("xck,xj->ckj", x_imag, x_sin)
    full_imag = product("xck,xj->ckj", x_imag, x_cos) - product("xck,xj->ckj", x_real, x_sin)
    kept_green = jnp.transpose(green[:, :, 0::2], (2, 1, 0))
    nyquist_green = jnp.transpose(green[:, :, 1], (1, 0))
    prod_real = kept_green * full_real
    prod_imag = kept_green * full_imag
    first_block = lax.axis_index("gx") * size_gz + lax.axis_index("gz") == 0
    first_slab = lax.axis_index("gy") == 0
    base_real = full_real[0]
    base_imag = full_imag[0]
    mirror_real = mirror_plane(base_real, first_block)
    mirror_imag = mirror_plane(base_imag, first_block)
    zero_real = 0.5 * (base_real + mirror_real)
    zero_imag = 0.5 * (base_imag - mirror_imag)
    nyq_real = 0.5 * (base_imag + mirror_imag)
    nyq_imag = 0.5 * (mirror_real - base_real)
    zero_green = kept_green[0]
    packed_real = zero_green * zero_real - nyquist_green * nyq_imag
    packed_imag = zero_green * zero_imag + nyquist_green * nyq_real
    slot_mask = jnp.logical_and(lax.iota(jnp.int32, prod_real.shape[0]) == 0, first_slab)
    prod_real = jnp.where(slot_mask[:, None, None], packed_real[None], prod_real)
    prod_imag = jnp.where(slot_mask[:, None, None], packed_imag[None], prod_imag)
    inv_xcos, inv_xsin = phase_table(
        lax.iota(jnp.int32, long_x), lax.iota(jnp.int32, grid_x), long_x
    )
    back_real = (
        product("ckj,jx->ckx", prod_real, inv_xcos) - product("ckj,jx->ckx", prod_imag, inv_xsin)
    ) / long_x
    back_imag = (
        product("ckj,jx->ckx", prod_imag, inv_xcos) + product("ckj,jx->ckx", prod_real, inv_xsin)
    ) / long_x
    mid_real, mid_imag = (
        lax.all_to_all(back_real, ("gx", "gz"), split_axis=2, concat_axis=1, tiled=True),
        lax.all_to_all(back_imag, ("gx", "gz"), split_axis=2, concat_axis=1, tiled=True),
    )
    y_order = lax.iota(jnp.int32, long_y)
    inv_ycos, inv_ysin = phase_table(
        pair_frequency(y_order, long_y), lax.iota(jnp.int32, grid_y), long_y
    )
    half_real = (
        product("cja,jy->cay", mid_real, inv_ycos) - product("cja,jy->cay", mid_imag, inv_ysin)
    ) / long_y
    half_imag = (
        product("cja,jy->cay", mid_imag, inv_ycos) + product("cja,jy->cay", mid_real, inv_ysin)
    ) / long_y
    last_real, last_imag = (
        lax.all_to_all(half_real, "gy", split_axis=2, concat_axis=0, tiled=True),
        lax.all_to_all(half_imag, "gy", split_axis=2, concat_axis=0, tiled=True),
    )
    kept_freq = lax.iota(jnp.int32, long_z // 2)
    base_cos, base_sin = phase_table(kept_freq, cell_z, long_z)
    inv_zcos = jnp.where(kept_freq[:, None] == 0, 1.0, 2.0 * base_cos)
    inv_zsin = jnp.where(kept_freq[:, None] == 0, -parity_sign[None, :], 2.0 * base_sin)
    result = (
        product("jab,jn->abn", last_real, inv_zcos) - product("jab,jn->abn", last_imag, inv_zsin)
    ) / long_z
    return lax.all_to_all(result, "gz", split_axis=2, concat_axis=0, tiled=True)


def solution(mesh):
    step = jax.shard_map(
        per_device,
        mesh=mesh,
        in_specs=(P("gx", "gy", "gz"), P(None, ("gx", "gz"), "gy")),
        out_specs=P("gx", "gy", "gz"),
        check_vma=False,
    )
    return step
```

```python
import functools
import math

import jax
import jax.numpy as jnp
import ml_dtypes
import numpy as np
from jax import lax
from jax.experimental import pallas as pl
from jax.experimental.pallas import tpu as pltpu
from jax.sharding import PartitionSpec as P

LANES = 128
PARTS = 2
CHUNKS = 4
VMEM_BYTES = 61 * 1024 * 1024


def np_halves(table):
    high = table.astype(np.float32).astype(ml_dtypes.bfloat16)
    low = (table - high.astype(np.float64)).astype(np.float32).astype(ml_dtypes.bfloat16)
    return np.stack([high, low])


def split(value):
    high = value.astype(jnp.bfloat16)
    return high, (value - high.astype(jnp.float32)).astype(jnp.bfloat16)


def mm(left, right):
    return jnp.dot(left, right, preferred_element_type=jnp.float32)


def table_left(high, low, value):
    v_high, v_low = split(value)
    both = mm(high, jnp.concatenate([v_high, v_low], axis=1))
    width = value.shape[1]
    return both[:, :width] + (both[:, width:] + mm(low, v_high))


def table_right(value, high, low):
    v_high, v_low = split(value)
    return mm(v_high, high) + (mm(v_low, high) + mm(v_high, low))


def block_swap(pieces, width):
    count = len(pieces)
    group = lax.broadcasted_iota(jnp.int32, pieces[0].shape, 1) // width
    out = []
    for c in range(count):
        total = None
        for g in range(count):
            moved = pieces[g]
            shift = (g - c) * width % LANES
            if shift:
                moved = pltpu.roll(moved, shift, 1)
            total = moved if total is None else jnp.where(group == g, moved, total)
        out.append(total)
    return out


def y_tables(length_y, blocks, units, scale):
    cells = np.arange(length_y // 2)
    freq = np.arange(length_y // 2)
    angle = 2.0 * np.pi * (np.outer(freq, cells) % length_y) / length_y
    sign = 1.0 - 2.0 * (cells % 2)
    real, imag = np.cos(angle), -np.sin(angle)
    imag[0] = sign
    weight = np.where(freq == 0, 1.0, 2.0)[:, None] * (scale / length_y)
    both = np.stack([real, imag], axis=1)
    back = both * weight[:, None]

    def ordered(table):
        table = table.reshape(blocks, 2, units, 2, -1)[:, :, ::-1]
        table = table.reshape(blocks, 2, PARTS, units // PARTS, 2, -1)
        return table.transpose(1, 2, 0, 3, 4, 5).reshape(2, length_y // 2, -1)

    forward = np.swapaxes(np_halves(ordered(both)), 0, 1)
    backward = np.swapaxes(np_halves(np.swapaxes(ordered(back), 1, 2)), 0, 1)
    return forward, backward


def x_table(length_x, group, rows):
    freqs = np.arange(length_x // 4)[:, None]
    place = np.arange(length_x // 2)[None, :]
    a, q = place % rows, place // rows % 2
    b, block = place // (2 * rows) % group, place // (2 * rows * group)
    cells = (block * rows + a) * group + b
    out = []
    for member in range(4):
        angle = 2.0 * np.pi * ((4 * freqs + member) * cells % length_x) / length_x
        c, s = np.cos(angle), np.sin(angle)
        out.append(np.concatenate([np.where(q == 0, c, s), np.where(q == 0, -s, c)], 0))
    return np_halves(np.stack(out))


def z_table(length_z, parts):
    place = np.arange(length_z)
    unit, member = place // 2, place % 2
    freq = np.where(unit == 0, member * (length_z // 2), np.where(member == 0, unit, length_z - unit))
    cells = np.arange(length_z // 2)
    rows = []
    for freqs in np.split(freq, parts):
        angle = 2.0 * np.pi * (np.outer(cells, freqs) % length_z) / length_z
        rows.append(np.concatenate([np.cos(angle), -np.sin(angle)], 1))
    return np_halves(np.stack(rows))


def expand(source, out, back):
    size = source.shape[1] // 2
    for at in range(source.shape[0] // size):
        c = source[at * size : (at + 1) * size, :size].astype(jnp.float32)
        s = source[at * size : (at + 1) * size, size:].astype(jnp.float32)
        full = jnp.concatenate(
            [jnp.concatenate([c, s], axis=1), jnp.concatenate([-s, c], axis=1)], axis=0
        )
        out[at] = full.astype(jnp.bfloat16)
        back[at] = full.T.astype(jnp.bfloat16)


def transposed(source, back):
    size = source.shape[1]
    for at in range(source.shape[0] // size):
        block = source[at * size : (at + 1) * size, :]
        back[at] = block.astype(jnp.float32).T.astype(jnp.bfloat16)


def whole_kernel(
    size_gx, size_gz, units,
    source_hbm, green_hbm, tables_hbm, out_ref,
    source, green, y_both, x_tab, x_back, z_half, z_tab, z_back,
    raw_own, raw_other, green_own, green_sent, green_other, nyquist, distant,
    f_sent, f_got, b_sent, b_got, lines, spectrum, part_own, part_sent, part_other,
    local_sem, send_sem, raw_sem, green_sem, f_sem, b_sem, part_sem,
):
    gx, gy, gz = lax.axis_index("gx"), lax.axis_index("gy"), lax.axis_index("gz")
    blocks = size_gx * size_gz
    block = gx * size_gz + gz
    group = size_gz
    width = LANES // group
    rows = raw_own.shape[1]
    count_y = raw_own.shape[2]
    lines_y = 2 * count_y
    each = units // PARTS
    piece = 2 * each * rows
    share = green_own.shape[3]
    quarter = green_own.shape[2]
    half_x = 2 * quarter
    positions = 4 * units
    partner = {"gy": 1 - gy}
    lower = gy == 0
    packed = block + gy == 0

    def remote(source_at, target_at, sent, got, device):
        return pltpu.make_async_remote_copy(
            source_at, target_at, send_sem.at[sent], got,
            device_id=device, device_id_type=pl.DeviceIdType.MESH,
        )

    def plane_device(step):
        target = lax.rem(block + step, blocks)
        return target, {"gx": target // size_gz, "gz": lax.rem(target, size_gz)}

    def span(part, chunk, at):
        start = ((part * CHUNKS + chunk) * blocks + at) * piece
        return pl.ds(pl.multiple_of(start, 8), piece)

    def send_plane(sent_ref, got_ref, which, sems, part, chunk):
        def body(step, _):
            target, device = plane_device(step)
            remote(
                sent_ref.at[span(part, chunk, target), :],
                got_ref.at[span(part, chunk, block), :],
                which, sems.at[part, chunk], device,
            ).start()
            return 0

        lax.fori_loop(1, blocks, body, 0)
        got_ref[span(part, chunk, block), :] = sent_ref[span(part, chunk, block), :]

    def wait_plane(got_ref, which, sems, part, chunk):
        everything = got_ref.at[pl.ds(0, (blocks - 1) * piece), :]
        remote(everything, everything, which, sems.at[part, chunk], partner).wait_recv()

    step_x = rows * group
    copies = [
        pltpu.make_async_copy(
            source_hbm.at[pl.ds(c * step_x, step_x)], source.at[pl.ds(c * step_x, step_x)], local_sem.at[c]
        )
        for c in range(CHUNKS)
    ]
    copies.append(pltpu.make_async_copy(green_hbm, green, local_sem.at[CHUNKS]))
    start = 0
    for n, (table, which) in enumerate(((x_tab, None), (z_half, None), (y_both, gy))):
        size = table.shape[0]
        at = start if which is None else start + which * size
        copies.append(
            pltpu.make_async_copy(
                tables_hbm.at[pl.ds(at, size), :], table, local_sem.at[CHUNKS + 1 + n]
            )
        )
        start += size
    for copy in copies:
        copy.start()

    barrier = pltpu.get_barrier_semaphore()

    def greet(step, _):
        _, device = plane_device(step)
        pl.semaphore_signal(barrier, inc=1, device_id=device, device_id_type=pl.DeviceIdType.MESH)
        return 0

    pl.semaphore_signal(barrier, inc=1, device_id=partner, device_id_type=pl.DeviceIdType.MESH)
    lax.fori_loop(1, blocks, greet, 0)

    for c in range(CHUNKS):
        copies[c].wait()
        for a in range(rows):
            at = (c * rows + a) * group
            raw_own[c, a] = jnp.concatenate([source[at + b] for b in range(group)], axis=0).T
        if c == 0:
            pl.semaphore_wait(barrier, blocks)
        for a in range(rows):
            remote(raw_own.at[c, a], raw_other.at[c, a], 0, raw_sem.at[c, a], partner).start()

    copies[CHUNKS].wait()

    def extract(step, _):
        u, m = step // 4, lax.rem(step, 4)
        for half, out in ((gy, green_own), (1 - gy, green_sent)):
            at = m * positions + 2 * (half * units + units - 1 - u)
            out[u, m] = green[pl.ds(at, quarter, stride=4 * positions), :]
        return 0

    lax.fori_loop(0, 4 * units, extract, 0)
    for m in range(4):
        nyquist[m] = green[pl.ds(m * positions + 1, quarter, stride=4 * positions), :]
    def green_copy(u):
        return remote(green_sent.at[u], green_other.at[u], 2, green_sem.at[u], partner)

    distant_copy = remote(nyquist, distant, 3, green_sem.at[units], partner)
    for u in range(units):
        green_copy(u).start()

    @pl.when(block + (1 - gy) == 0)
    def _():
        distant_copy.start()

    copies[CHUNKS + 1].wait()
    transposed(x_tab, x_back)
    copies[CHUNKS + 2].wait()
    expand(z_half, z_tab, z_back)
    copies[CHUNKS + 3].wait()

    def transform(c):
        def body(a, _):
            remote(raw_own.at[c, a], raw_other.at[c, a], 0, raw_sem.at[c, a], partner).wait_recv()
            own, other = raw_own[c, a], raw_other[c, a]
            cells = jnp.concatenate([jnp.where(lower, own, other), jnp.where(lower, other, own)], axis=0)
            freqs = table_left(y_both[:lines_y, :lines_y], y_both[lines_y:, :lines_y], cells)
            count = blocks * 2 * each
            for part in range(PARTS):
                start = (part * CHUNKS + c) * blocks * piece + a
                f_sent[pl.ds(start, count, stride=rows), :] = freqs[part * count : (part + 1) * count]
            return 0

        lax.fori_loop(0, rows, body, 0)

    for c in range(CHUNKS):
        transform(c)
        send_plane(f_sent, f_got, 1, f_sem, 0, c)
    for part in range(1, PARTS):
        for c in range(CHUNKS):
            send_plane(f_sent, f_got, 1, f_sem, part, c)

    def turned(value):
        tiles = value.reshape(-1, 2 * rows, LANES)
        real = lax.broadcasted_iota(jnp.int32, tiles.shape, 1) < rows
        moved = pltpu.roll(tiles, rows, 1)
        return jnp.where(real, moved, -moved).reshape(value.shape)

    def forward(field):
        near, far = field[:half_x], field[half_x:]
        twist = turned(far)
        out = []
        for m, cells in enumerate((near + far, near + twist, near - far, near - twist)):
            high, low = (x_tab[(4 * part + m) * half_x : (4 * part + m + 1) * half_x, :] for part in range(2))
            o = table_left(high, low, cells)
            out.append(jnp.concatenate([o[:quarter], o[quarter:]], axis=1))
        out = jnp.concatenate(out, axis=0)
        return [table_right(out, z_tab[h], z_tab[2 + h]) for h in (gy, 1 - gy)]

    def unit_step(u, _):
        part, c = u // each, lax.rem(u, each)
        here = jnp.logical_and(packed, u == units - 1)

        @pl.when(c == 0)
        def _():
            for chunk in range(CHUNKS):
                wait_plane(f_got, 1, f_sem, part, chunk)

        def place(chunk, at):
            start = ((part * CHUNKS + chunk) * blocks + at) * piece + 2 * c * rows
            return pl.ds(pl.multiple_of(start, 8), 2 * rows)

        for x in range(size_gx):
            for chunk in range(CHUNKS):
                pieces = [f_got[place(chunk, x * size_gz + g), :] for g in range(size_gz)]
                at = (x * CHUNKS + chunk) * 2 * step_x
                for b, moved in enumerate(block_swap(pieces, width)):
                    lines[at + 2 * b * rows : at + 2 * (b + 1) * rows] = moved

        def masked(keep_real):
            field = lines[...]
            tiles = field.reshape(-1, 2 * rows, LANES)
            real = lax.broadcasted_iota(jnp.int32, tiles.shape, 1) < rows
            keep = jnp.logical_or(real == keep_real, jnp.logical_not(here))
            return jnp.where(keep, tiles, 0.0).reshape(field.shape)

        freqs = forward(masked(True))
        green_copy(u).wait_recv()
        for side, gains in enumerate((green_own, green_other)):
            gain = gains[u].reshape(4 * quarter, share)
            spectrum[side] = jnp.concatenate([gain, gain], axis=1) * freqs[side]

        @pl.when(here)
        def _():
            more = forward(masked(False))
            distant_copy.wait_recv()
            for side, freqs in enumerate(more):
                gain = (nyquist, distant)[side][...].reshape(4 * quarter, share)
                spectrum[side] += jnp.concatenate([gain, gain], axis=1) * freqs

        inverse = sum(
            table_right(spectrum[side], z_back[h], z_back[2 + h]) for side, h in ((0, gy), (1, 1 - gy))
        )
        cells = []
        for m in range(4):
            out = inverse[m * quarter : (m + 1) * quarter]
            both = jnp.concatenate([out[:, :LANES], out[:, LANES:]], axis=0)
            cells.append(table_left(x_back[m], x_back[4 + m], both))
        even, odd = cells[0] + cells[2], cells[1] + cells[3]
        lines[:half_x] = even + odd
        lines[half_x:] = (cells[0] - cells[2]) - turned(cells[1] - cells[3])

        for x in range(size_gx):
            for chunk in range(CHUNKS):
                at = (x * CHUNKS + chunk) * 2 * step_x
                pieces = [lines[at + 2 * b * rows : at + 2 * (b + 1) * rows] for b in range(group)]
                for g, moved in enumerate(block_swap(pieces, width)):
                    b_sent[place(chunk, x * size_gz + g), :] = moved

        @pl.when(c == each - 1)
        def _():
            for chunk in range(CHUNKS):
                send_plane(b_sent, b_got, 4, b_sem, part, chunk)

        return 0

    lax.fori_loop(0, units, unit_step, 0)

    def part_copy(c, a):
        return remote(part_sent.at[c, a], part_other.at[c, a], 5, part_sem.at[c, a], partner)

    def invert(c):
        for part in range(PARTS):
            wait_plane(b_got, 4, b_sem, part, c)

        def body(a, _):
            count = blocks * 2 * each
            freqs = jnp.concatenate(
                [
                    b_got[pl.ds((part * CHUNKS + c) * blocks * piece + a, count, stride=rows), :]
                    for part in range(PARTS)
                ],
                axis=0,
            )
            cells = table_left(y_both[:lines_y, lines_y:], y_both[lines_y:, lines_y:], freqs)
            low, high = cells[:count_y], cells[count_y:]
            part_sent[c, a] = jnp.where(lower, high, low)
            part_own[c, a] = jnp.where(lower, low, high)
            part_copy(c, a).start()
            return 0

        lax.fori_loop(0, rows, body, 0)

    for c in range(CHUNKS):
        invert(c)

    for c in range(CHUNKS):
        def finish(a, _):
            part_copy(c, a).wait_recv()
            cells = (part_own[c, a] + part_other[c, a]).T
            for b in range(group):
                out_ref[(c * rows + a) * group + b] = cells[b * width : (b + 1) * width]
            return 0

        lax.fori_loop(0, rows, finish, 0)


    remote(raw_own, raw_other, 0, raw_sem.at[0, 0], partner).wait_send()
    moved = f_sent.at[pl.ds(0, PARTS * CHUNKS * (blocks - 1) * piece), :]
    remote(moved, moved, 1, f_sem.at[0, 0], partner).wait_send()
    remote(green_sent, green_other, 2, green_sem.at[0], partner).wait_send()

    @pl.when(block + (1 - gy) == 0)
    def _():
        distant_copy.wait_send()

    remote(moved, moved, 4, b_sem.at[0, 0], partner).wait_send()
    remote(part_sent, part_other, 5, part_sem.at[0, 0], partner).wait_send()


def f32(*shape):
    return jax.ShapeDtypeStruct(shape, jnp.float32)


def fast_device(source, green):
    size_gx = lax.axis_size("gx")
    size_gy = lax.axis_size("gy")
    size_gz = lax.axis_size("gz")
    brick_x, brick_y, brick_z = source.shape
    long_x, places, share = green.shape
    long_y = 2 * brick_y * size_gy
    long_z = 2 * brick_z * size_gz
    blocks = size_gx * size_gz
    units = places // (2 * size_gy)
    group = LANES // brick_z
    rows = brick_x // group // CHUNKS
    quarter = long_x // 4
    y_tab, y_back = y_tables(long_y, blocks, units, 1.0 / (long_x * long_z))
    x_tab, z_tab = x_table(long_x, group, rows), z_table(long_z, 2)
    flat = lambda table: table.reshape(-1, 2 * share)
    y_both = np.concatenate([y_tab, y_back], axis=3)
    tables = np.concatenate([flat(x_tab), flat(z_tab), flat(y_both)])
    lines = blocks * units * 2 * CHUNKS * rows
    vmem = lambda *shape: pltpu.VMEM(shape, jnp.float32)
    half = lambda *shape: pltpu.VMEM(shape, jnp.bfloat16)
    raw = (CHUNKS, rows, brick_y, LANES)
    slots = (units, 4, quarter, share)
    result = pl.pallas_call(
        functools.partial(whole_kernel, size_gx, size_gz, units),
        out_shape=pltpu.VMEM((brick_x, brick_z, brick_y), jnp.float32),
        in_specs=[pl.BlockSpec(memory_space=pltpu.HBM)] * 3,
        out_specs=pl.BlockSpec(memory_space=pltpu.VMEM),
        scratch_shapes=[
            vmem(brick_x, brick_z, brick_y),
            vmem(long_x * places, share),
            half(*flat(y_both[0]).shape),
            half(*flat(x_tab).shape),
            half(8, 2 * quarter, 2 * quarter),
            half(*flat(z_tab).shape),
            half(4, long_z, 2 * share),
            half(4, long_z, 2 * share),
            vmem(*raw),
            vmem(*raw),
            vmem(*slots),
            vmem(*slots),
            vmem(*slots),
            vmem(*slots[1:]),
            vmem(*slots[1:]),
            vmem(lines, LANES),
            vmem(lines, LANES),
            vmem(lines, LANES),
            vmem(lines, LANES),
            vmem(long_x, LANES),
            vmem(2, long_x, 2 * share),
            vmem(*raw),
            vmem(*raw),
            vmem(*raw),
            pltpu.SemaphoreType.DMA((CHUNKS + 4,)),
            pltpu.SemaphoreType.DMA((6,)),
            pltpu.SemaphoreType.DMA((CHUNKS, rows)),
            pltpu.SemaphoreType.DMA((units + 1,)),
            pltpu.SemaphoreType.DMA((PARTS, CHUNKS)),
            pltpu.SemaphoreType.DMA((PARTS, CHUNKS)),
            pltpu.SemaphoreType.DMA((CHUNKS, rows)),
        ],
        compiler_params=pltpu.CompilerParams(
            vmem_limit_bytes=VMEM_BYTES, collective_id=0, has_side_effects=True
        ),
    )(jnp.swapaxes(source, 1, 2), green.reshape(long_x * places, share), tables)
    return jnp.swapaxes(result, 1, 2)


def fits(sizes, source, green):
    brick_x, brick_y, brick_z = source.shape
    units = green.shape[1] // (2 * sizes["gy"])
    return (
        brick_z * sizes["gz"] == LANES
        and green.shape[2] == LANES
        and sizes["gx"] * brick_x == 2 * LANES
        and brick_y * sizes["gy"] == LANES
        and brick_x * brick_z == 4 * CHUNKS * LANES
        and units % PARTS == 0
        and sizes["gy"] == 2
    )


def phase_table(row_index, column_index, length):
    phase_index = row_index[:, None] * column_index[None, :] % length
    angles = phase_index.astype(jnp.float32) * (2.0 * math.pi / length)
    return (jnp.cos(angles), jnp.sin(angles))


def pair_frequency(position, length):
    unit_index = position // 2
    member = position % 2
    return jnp.where(
        unit_index == 0,
        member * (length // 2),
        jnp.where(member == 0, unit_index, length - unit_index),
    )


def product(form, left, table):
    return jnp.einsum(form, left, table, precision=lax.Precision.HIGHEST)


def mirror_plane(field, first_block):
    flipped = jnp.roll(jnp.flip(field, 1), 1, 1)
    count_y, count_x = field.shape
    swapped = flipped.reshape(count_y // 2, 2, count_x)[:, ::-1, :].reshape(count_y, count_x)
    local_row = lax.iota(jnp.int32, count_y)
    keep_unit = jnp.logical_and(first_block, local_row < 2)
    return jnp.where(keep_unit[:, None], flipped, swapped)


def per_device(source, green):
    size_gx = lax.axis_size("gx")
    size_gy = lax.axis_size("gy")
    size_gz = lax.axis_size("gz")
    brick_x, brick_y, brick_z = source.shape
    if fits({"gx": size_gx, "gy": size_gy, "gz": size_gz}, source, green):
        return fast_device(source, green)
    grid_x = brick_x * size_gx
    grid_y = brick_y * size_gy
    grid_z = brick_z * size_gz
    long_x = 2 * grid_x
    long_y = 2 * grid_y
    long_z = 2 * grid_z
    cell_z = lax.iota(jnp.int32, grid_z)
    parity_sign = (1 - 2 * (cell_z % 2)).astype(jnp.float32)
    z_lines = lax.all_to_all(source, "gz", split_axis=0, concat_axis=2, tiled=True)
    kept_freq = lax.iota(jnp.int32, long_z // 2)
    z_cos, z_sin = phase_table(cell_z, kept_freq, long_z)
    z_sin = jnp.where(kept_freq[None, :] == 0, -parity_sign[:, None], z_sin)
    z_real = product("abn,nk->abk", z_lines, z_cos)
    z_imag = -product("abn,nk->abk", z_lines, z_sin)
    y_real, y_imag = (
        lax.all_to_all(z_real, "gy", split_axis=2, concat_axis=1, tiled=True),
        lax.all_to_all(z_imag, "gy", split_axis=2, concat_axis=1, tiled=True),
    )
    y_cos, y_sin = phase_table(
        lax.iota(jnp.int32, grid_y), pair_frequency(lax.iota(jnp.int32, long_y), long_y), long_y
    )
    fy_real = product("ayc,yk->ack", y_real, y_cos) + product("ayc,yk->ack", y_imag, y_sin)
    fy_imag = product("ayc,yk->ack", y_imag, y_cos) - product("ayc,yk->ack", y_real, y_sin)
    x_real, x_imag = (
        lax.all_to_all(fy_real, ("gx", "gz"), split_axis=2, concat_axis=0, tiled=True),
        lax.all_to_all(fy_imag, ("gx", "gz"), split_axis=2, concat_axis=0, tiled=True),
    )
    x_rows = lax.iota(jnp.int32, grid_x)
    x_cos, x_sin = phase_table(x_rows, lax.iota(jnp.int32, long_x), long_x)
    full_real = product("xck,xj->ckj", x_real, x_cos) + product("xck,xj->ckj", x_imag, x_sin)
    full_imag = product("xck,xj->ckj", x_imag, x_cos) - product("xck,xj->ckj", x_real, x_sin)
    kept_green = jnp.transpose(green[:, :, 0::2], (2, 1, 0))
    nyquist_green = jnp.transpose(green[:, :, 1], (1, 0))
    prod_real = kept_green * full_real
    prod_imag = kept_green * full_imag
    first_block = lax.axis_index("gx") * size_gz + lax.axis_index("gz") == 0
    first_slab = lax.axis_index("gy") == 0
    base_real = full_real[0]
    base_imag = full_imag[0]
    mirror_real = mirror_plane(base_real, first_block)
    mirror_imag = mirror_plane(base_imag, first_block)
    zero_real = 0.5 * (base_real + mirror_real)
    zero_imag = 0.5 * (base_imag - mirror_imag)
    nyq_real = 0.5 * (base_imag + mirror_imag)
    nyq_imag = 0.5 * (mirror_real - base_real)
    zero_green = kept_green[0]
    packed_real = zero_green * zero_real - nyquist_green * nyq_imag
    packed_imag = zero_green * zero_imag + nyquist_green * nyq_real
    slot_mask = jnp.logical_and(lax.iota(jnp.int32, prod_real.shape[0]) == 0, first_slab)
    prod_real = jnp.where(slot_mask[:, None, None], packed_real[None], prod_real)
    prod_imag = jnp.where(slot_mask[:, None, None], packed_imag[None], prod_imag)
    inv_xcos, inv_xsin = phase_table(
        lax.iota(jnp.int32, long_x), lax.iota(jnp.int32, grid_x), long_x
    )
    back_real = (
        product("ckj,jx->ckx", prod_real, inv_xcos) - product("ckj,jx->ckx", prod_imag, inv_xsin)
    ) / long_x
    back_imag = (
        product("ckj,jx->ckx", prod_imag, inv_xcos) + product("ckj,jx->ckx", prod_real, inv_xsin)
    ) / long_x
    mid_real, mid_imag = (
        lax.all_to_all(back_real, ("gx", "gz"), split_axis=2, concat_axis=1, tiled=True),
        lax.all_to_all(back_imag, ("gx", "gz"), split_axis=2, concat_axis=1, tiled=True),
    )
    y_order = lax.iota(jnp.int32, long_y)
    inv_ycos, inv_ysin = phase_table(
        pair_frequency(y_order, long_y), lax.iota(jnp.int32, grid_y), long_y
    )
    half_real = (
        product("cja,jy->cay", mid_real, inv_ycos) - product("cja,jy->cay", mid_imag, inv_ysin)
    ) / long_y
    half_imag = (
        product("cja,jy->cay", mid_imag, inv_ycos) + product("cja,jy->cay", mid_real, inv_ysin)
    ) / long_y
    last_real, last_imag = (
        lax.all_to_all(half_real, "gy", split_axis=2, concat_axis=0, tiled=True),
        lax.all_to_all(half_imag, "gy", split_axis=2, concat_axis=0, tiled=True),
    )
    kept_freq = lax.iota(jnp.int32, long_z // 2)
    base_cos, base_sin = phase_table(kept_freq, cell_z, long_z)
    inv_zcos = jnp.where(kept_freq[:, None] == 0, 1.0, 2.0 * base_cos)
    inv_zsin = jnp.where(kept_freq[:, None] == 0, -parity_sign[None, :], 2.0 * base_sin)
    result = (
        product("jab,jn->abn", last_real, inv_zcos) - product("jab,jn->abn", last_imag, inv_zsin)
    ) / long_z
    return lax.all_to_all(result, "gz", split_axis=2, concat_axis=0, tiled=True)


def solution(mesh):
    step = jax.shard_map(
        per_device,
        mesh=mesh,
        in_specs=(P("gx", "gy", "gz"), P(None, ("gx", "gz"), "gy")),
        out_specs=P("gx", "gy", "gz"),
        check_vma=False,
    )
    return step
```

```python
import functools
import math

import jax
import jax.numpy as jnp
import ml_dtypes
import numpy as np
from jax import lax
from jax.experimental import pallas as pl
from jax.experimental.pallas import tpu as pltpu
from jax.sharding import PartitionSpec as P

LANES = 128
PARTS = 2
CHUNKS = 8
SENT = (3,5,6,7,8,8,8,8,8,8)
VMEM_BYTES = 61 * 1024 * 1024


def np_halves(table):
    high = table.astype(np.float32).astype(ml_dtypes.bfloat16)
    low = (table - high.astype(np.float64)).astype(np.float32).astype(ml_dtypes.bfloat16)
    return np.stack([high, low])


def split(value):
    high = value.astype(jnp.bfloat16)
    return high, (value - high.astype(jnp.float32)).astype(jnp.bfloat16)


def mm(left, right):
    return jnp.dot(left, right, preferred_element_type=jnp.float32)


def table_left(high, low, value):
    v_high, v_low = split(value)
    both = mm(high, jnp.concatenate([v_high, v_low], axis=1))
    width = value.shape[1]
    return both[:, :width] + (both[:, width:] + mm(low, v_high))


def table_right(value, high, low):
    v_high, v_low = split(value)
    return mm(v_high, high) + (mm(v_low, high) + mm(v_high, low))


def block_swap(pieces, width):
    count = len(pieces)
    group = lax.broadcasted_iota(jnp.int32, pieces[0].shape, 1) // width
    out = []
    for c in range(count):
        total = None
        for g in range(count):
            moved = pieces[g]
            shift = (g - c) * width % LANES
            if shift:
                moved = pltpu.roll(moved, shift, 1)
            total = moved if total is None else jnp.where(group == g, moved, total)
        out.append(total)
    return out


def y_tables(length_y, blocks, units, scale):
    cells = np.arange(length_y // 2)
    freq = np.arange(length_y // 2)
    angle = 2.0 * np.pi * (np.outer(freq, cells) % length_y) / length_y
    sign = 1.0 - 2.0 * (cells % 2)
    real, imag = np.cos(angle), -np.sin(angle)
    imag[0] = sign
    weight = np.where(freq == 0, 1.0, 2.0)[:, None] * (scale / length_y)
    both = np.stack([real, imag], axis=1)
    back = both * weight[:, None]

    def ordered(table):
        table = table.reshape(blocks, 2, units, 2, -1)[:, :, ::-1]
        table = table.reshape(blocks, 2, PARTS, units // PARTS, 2, -1)
        return table.transpose(1, 2, 0, 3, 4, 5).reshape(2, length_y // 2, -1)

    forward = np.swapaxes(np_halves(ordered(both)), 0, 1)
    backward = np.swapaxes(np_halves(np.swapaxes(ordered(back), 1, 2)), 0, 1)
    return forward, backward


def x_table(length_x, group, rows):
    freqs = np.arange(length_x // 4)[:, None]
    place = np.arange(length_x // 2)[None, :]
    a, q, h = place % rows, place // rows % 2, place // (2 * rows) % 2
    b, block = place // (4 * rows) % group, place // (4 * rows * group)
    cells = ((2 * block + h) * rows + a) * group + b
    out = []
    for member in range(4):
        angle = 2.0 * np.pi * ((4 * freqs + member) * cells % length_x) / length_x
        c, s = np.cos(angle), np.sin(angle)
        out.append(np.concatenate([np.where(q == 0, c, s), np.where(q == 0, -s, c)], 0))
    return np_halves(np.stack(out))


def z_table(length_z, parts):
    place = np.arange(length_z)
    unit, member = place // 2, place % 2
    freq = np.where(unit == 0, member * (length_z // 2), np.where(member == 0, unit, length_z - unit))
    cells = np.arange(length_z // 2)
    rows = []
    for freqs in np.split(freq, parts):
        angle = 2.0 * np.pi * (np.outer(cells, freqs) % length_z) / length_z
        rows.append(np.concatenate([np.cos(angle), -np.sin(angle)], 1))
    return np_halves(np.stack(rows))


def expand(source, out, back):
    size = source.shape[1] // 2
    for at in range(source.shape[0] // size):
        c = source[at * size : (at + 1) * size, :size].astype(jnp.float32)
        s = source[at * size : (at + 1) * size, size:].astype(jnp.float32)
        full = jnp.concatenate(
            [jnp.concatenate([c, s], axis=1), jnp.concatenate([-s, c], axis=1)], axis=0
        )
        out[at] = full.astype(jnp.bfloat16)
        back[at] = full.T.astype(jnp.bfloat16)


def transposed(source, back):
    size = source.shape[1]
    for at in range(source.shape[0] // size):
        block = source[at * size : (at + 1) * size, :]
        back[at] = block.astype(jnp.float32).T.astype(jnp.bfloat16)


def whole_kernel(
    size_gx, size_gz, units,
    source_hbm, green_hbm, tables_hbm, out_ref,
    source, green, y_both, x_tab, x_back, z_half, z_tab, z_back,
    raw_own, raw_other, green_own, green_sent, green_other, nyquist, distant,
    f_sent, f_got, b_sent, b_got, lines, extra, spectrum, part_own, part_sent, part_other,
    local_sem, send_sem, raw_sem, green_sem, f_sem, b_sem, part_sem,
):
    gx, gy, gz = lax.axis_index("gx"), lax.axis_index("gy"), lax.axis_index("gz")
    blocks = size_gx * size_gz
    block = gx * size_gz + gz
    group = size_gz
    width = LANES // group
    rows = raw_own.shape[1]
    count_y = raw_own.shape[2]
    lines_y = 2 * count_y
    each = units // PARTS
    piece = 2 * each * rows
    share = green_own.shape[3]
    quarter = green_own.shape[2]
    half_x = 2 * quarter
    positions = 4 * units
    partner = {"gy": 1 - gy}
    lower = gy == 0
    packed = block + gy == 0

    def remote(source_at, target_at, sent, got, device):
        return pltpu.make_async_remote_copy(
            source_at, target_at, send_sem.at[sent], got,
            device_id=device, device_id_type=pl.DeviceIdType.MESH,
        )

    def plane_device(step):
        target = lax.rem(block + step, blocks)
        return target, {"gx": target // size_gz, "gz": lax.rem(target, size_gz)}

    def send_plane(sent_ref, got_ref, which, sems, part, chunk, count):
        at = pl.ds(part * CHUNKS + chunk, count)

        def body(step, _):
            target, device = plane_device(step)
            remote(
                sent_ref.at[at, target], got_ref.at[at, block], which, sems.at[part, chunk], device
            ).start()
            return 0

        lax.fori_loop(1, blocks, body, 0)
        got_ref[at, block] = sent_ref[at, block]

    def wait_plane(got_ref, which, sems, part, chunk, count):
        everything = got_ref.at[pl.ds(0, count), pl.ds(0, blocks - 1)]
        remote(everything, everything, which, sems.at[part, chunk], partner).wait_recv()

    flat = lambda ref: ref.reshape(PARTS * CHUNKS * blocks * piece, LANES)
    step_x = rows * group
    copies = [
        pltpu.make_async_copy(
            source_hbm.at[pl.ds(c * step_x, step_x)], source.at[pl.ds(c * step_x, step_x)], local_sem.at[c]
        )
        for c in range(CHUNKS)
    ]
    copies.append(pltpu.make_async_copy(green_hbm, green, local_sem.at[CHUNKS]))
    start = 0
    for n, (table, which) in enumerate(((x_tab, None), (z_half, None), (y_both, gy))):
        size = table.shape[0]
        at = start if which is None else start + which * size
        copies.append(
            pltpu.make_async_copy(
                tables_hbm.at[pl.ds(at, size), :], table, local_sem.at[CHUNKS + 1 + n]
            )
        )
        start += size
    for copy in copies:
        copy.start()

    barrier = pltpu.get_barrier_semaphore()

    def greet(step, _):
        _, device = plane_device(step)
        pl.semaphore_signal(barrier, inc=1, device_id=device, device_id_type=pl.DeviceIdType.MESH)
        return 0

    pl.semaphore_signal(barrier, inc=1, device_id=partner, device_id_type=pl.DeviceIdType.MESH)
    lax.fori_loop(1, blocks, greet, 0)

    for c in range(CHUNKS):
        copies[c].wait()
        for a in range(rows):
            at = (c * rows + a) * group
            raw_own[c, a] = jnp.concatenate([source[at + b] for b in range(group)], axis=0).T
        if c == 0:
            pl.semaphore_wait(barrier, blocks)
        for a in range(rows):
            remote(raw_own.at[c, a], raw_other.at[c, a], 0, raw_sem.at[c, a], partner).start()

    copies[CHUNKS].wait()

    def extract(step, _):
        u, m = step // 4, lax.rem(step, 4)
        for half, out in ((gy, green_own), (1 - gy, green_sent)):
            at = m * positions + 2 * (half * units + units - 1 - u)
            out[u, m] = green[pl.ds(at, quarter, stride=4 * positions), :]
        return 0

    lax.fori_loop(0, 4 * units, extract, 0)
    for m in range(4):
        nyquist[m] = green[pl.ds(m * positions + 1, quarter, stride=4 * positions), :]
    def green_copy(u, sent=2):
        return remote(green_sent.at[u], green_other.at[u], sent, green_sem.at[u], partner)

    last = units - 1
    some = pl.ds(0, quarter // 2 + 8)
    plane_copy = remote(
        green_sent.at[last, :, some], green_other.at[last, :, some], 6, green_sem.at[last], partner
    )
    distant_copy = remote(nyquist.at[:, some], distant.at[:, some], 3, green_sem.at[units], partner)
    giver = block + (1 - gy) == 0

    for u in range(last):
        green_copy(u).start()

    @pl.when(giver)
    def _():
        distant_copy.start()
        plane_copy.start()

    @pl.when(jnp.logical_not(giver))
    def _():
        green_copy(last, 6).start()

    copies[CHUNKS + 1].wait()
    transposed(x_tab, x_back)
    copies[CHUNKS + 2].wait()
    expand(z_half, z_tab, z_back)
    copies[CHUNKS + 3].wait()

    def transform(c):
        def body(a, _):
            remote(raw_own.at[c, a], raw_other.at[c, a], 0, raw_sem.at[c, a], partner).wait_recv()
            own, other = raw_own[c, a], raw_other[c, a]
            cells = jnp.concatenate([jnp.where(lower, own, other), jnp.where(lower, other, own)], axis=0)
            freqs = table_left(y_both[:lines_y, :lines_y], y_both[lines_y:, :lines_y], cells)
            count = blocks * 2 * each
            for part in range(PARTS):
                start = (part * CHUNKS + c) * blocks * piece + a
                flat(f_sent)[pl.ds(start, count, stride=rows), :] = freqs[part * count : (part + 1) * count]
            return 0

        lax.fori_loop(0, rows, body, 0)

    for c in range(CHUNKS):
        transform(c)
        send_plane(f_sent, f_got, 1, f_sem, 0, c, 1)
    for part in range(1, PARTS):
        send_plane(f_sent, f_got, 1, f_sem, part, 0, CHUNKS)

    def tiled(value):
        tiles = value.reshape(-1, 8, LANES)
        return tiles, lax.broadcasted_iota(jnp.int32, tiles.shape, 1) // rows % 2 == 0

    def turned(value):
        tiles, real = tiled(value)
        return jnp.where(real, pltpu.roll(tiles, 8 - rows, 1), -pltpu.roll(tiles, rows, 1)).reshape(value.shape)

    def chosen(where_real, where_imag):
        left, real = tiled(where_real)
        return jnp.where(real, left, tiled(where_imag)[0]).reshape(where_real.shape)

    def forward(field):
        near, far = field[:half_x], field[half_x:]
        twist = turned(far)
        out = []
        for m, cells in enumerate((near + far, near + twist, near - far, near - twist)):
            high, low = (x_tab[(4 * part + m) * half_x : (4 * part + m + 1) * half_x, :] for part in range(2))
            o = table_left(high, low, cells)
            out.append(jnp.concatenate([o[:quarter], o[quarter:]], axis=1))
        out = jnp.concatenate(out, axis=0)
        return [table_right(out, z_tab[h], z_tab[2 + h]) for h in (gy, 1 - gy)]

    def solve(field, gains_of):
        freqs = forward(field)
        for side, gain in enumerate(gains_of()):
            gain = gain.reshape(4 * quarter, share)
            spectrum[side] = jnp.concatenate([gain, gain], axis=1) * freqs[side]
        inverse = sum(
            table_right(spectrum[side], z_back[h], z_back[2 + h]) for side, h in ((0, gy), (1, 1 - gy))
        )
        cells = []
        for m in range(4):
            out = inverse[m * quarter : (m + 1) * quarter]
            both = jnp.concatenate([out[:, :LANES], out[:, LANES:]], axis=0)
            cells.append(table_left(x_back[m], x_back[4 + m], both))
        even, odd = cells[0] + cells[2], cells[1] + cells[3]
        far = (cells[0] - cells[2]) - turned(cells[1] - cells[3])
        return jnp.concatenate([even + odd, far], axis=0)

    def folded(gain):
        m = lax.broadcasted_iota(jnp.int32, gain.shape, 0)
        freq = 4 * lax.broadcasted_iota(jnp.int32, gain.shape, 1) + m
        edge = jnp.logical_or(freq == 0, freq == 2 * quarter)
        return jnp.where(edge, gain, jnp.where(freq < 2 * quarter, 2.0 * gain, 0.0))

    def unit_step(part, c):
        u = part * each + c
        here = jnp.logical_and(packed, u == last)

        def gains():
            green_copy(u).wait_recv()
            return green_own[u], green_other[u]

        def plane_gains():
            plane_copy.wait_recv()
            return green_own[last], folded(green_other[last])

        def distant_gains():
            distant_copy.wait_recv()
            return nyquist[...], folded(distant[...])

        @pl.when(jnp.logical_not(here))
        def _():
            lines[c] = solve(lines[c], gains)

        @pl.when(here)
        def _():
            field = lines[last % each]
            zero = jnp.zeros_like(field)
            extra[...] = solve(chosen(zero, field), distant_gains)
            lines[last % each] = chosen(solve(chosen(lines[last % each], zero), plane_gains), extra[...])

    def part_step(part, _):
        @pl.when(part == 0)
        def _():
            for chunk in range(CHUNKS):
                wait_plane(f_got, 1, f_sem, 0, chunk, 1)

        @pl.when(part > 0)
        def _():
            wait_plane(f_got, 1, f_sem, part, 0, CHUNKS)

        first = lax.broadcasted_iota(jnp.int32, (8, LANES), 0) < 4
        for x in range(size_gx):
            for pair in range(CHUNKS // 2):
                moved = []
                for h in range(2):
                    at = part * CHUNKS + 2 * pair + h
                    moved.append(block_swap([f_got[at, x * size_gz + g] for g in range(size_gz)], width))
                for b, (left, right) in enumerate(zip(*moved)):
                    at = ((x * CHUNKS // 2 + pair) * group + b) * 8
                    lines[0, at : at + 8] = jnp.where(first, left, pltpu.roll(right, 4, 0))
                    lines[1, at : at + 8] = jnp.where(first, pltpu.roll(left, 4, 0), right)

        def body(c, _):
            unit_step(part, c)
            return 0

        lax.fori_loop(0, each, body, 0)

        for x in range(size_gx):
            for pair in range(CHUNKS // 2):
                sides = ([], [])
                for b in range(group):
                    at = ((x * CHUNKS // 2 + pair) * group + b) * 8
                    left, right = lines[0, at : at + 8], lines[1, at : at + 8]
                    sides[0].append(jnp.where(first, left, pltpu.roll(right, 4, 0)))
                    sides[1].append(jnp.where(first, pltpu.roll(left, 4, 0), right))
                for h in range(2):
                    at = part * CHUNKS + 2 * pair + h
                    for g, moved in enumerate(block_swap(sides[h], width)):
                        b_sent[at, x * size_gz + g] = moved

        @pl.when(part < PARTS - 1)
        def _():
            send_plane(b_sent, b_got, 4, b_sem, part, 0, CHUNKS)

        @pl.when(part == PARTS - 1)
        def _():
            for chunk in range(SENT[0]):
                send_plane(b_sent, b_got, 4, b_sem, part, chunk, 1)

        return 0

    lax.fori_loop(0, PARTS, part_step, 0)

    def send_more(step):
        for chunk in range(SENT[step], SENT[step + 1]):
            send_plane(b_sent, b_got, 4, b_sem, PARTS - 1, chunk, 1)

    def part_copy(c, a):
        return remote(part_sent.at[c, a], part_other.at[c, a], 5, part_sem.at[c, a], partner)

    def invert(c):
        wait_plane(b_got, 4, b_sem, PARTS - 1, c, 1)
        send_more(c + 1)

        def body(a, _):
            count = blocks * 2 * each
            freqs = jnp.concatenate(
                [
                    flat(b_got)[pl.ds((part * CHUNKS + c) * blocks * piece + a, count, stride=rows), :]
                    for part in range(PARTS)
                ],
                axis=0,
            )
            cells = table_left(y_both[:lines_y, lines_y:], y_both[lines_y:, lines_y:], freqs)
            low, high = cells[:count_y], cells[count_y:]
            part_sent[c, a] = jnp.where(lower, high, low)
            part_own[c, a] = jnp.where(lower, low, high)
            part_copy(c, a).start()
            return 0

        lax.fori_loop(0, rows, body, 0)

    for part in range(PARTS - 1):
        wait_plane(b_got, 4, b_sem, part, 0, CHUNKS)
    send_more(0)
    for c in range(CHUNKS):
        invert(c)

    for c in range(CHUNKS):
        def finish(a, _):
            part_copy(c, a).wait_recv()
            cells = (part_own[c, a] + part_other[c, a]).T
            for b in range(group):
                out_ref[(c * rows + a) * group + b] = cells[b * width : (b + 1) * width]
            return 0

        lax.fori_loop(0, rows, finish, 0)


    remote(raw_own, raw_other, 0, raw_sem.at[0, 0], partner).wait_send()
    moved = f_sent.at[:, pl.ds(0, blocks - 1)]
    remote(moved, moved, 1, f_sem.at[0, 0], partner).wait_send()
    remote(moved, moved, 4, b_sem.at[0, 0], partner).wait_send()
    most = green_sent.at[pl.ds(0, last)]
    remote(most, most, 2, green_sem.at[0], partner).wait_send()

    @pl.when(giver)
    def _():
        distant_copy.wait_send()
        plane_copy.wait_send()

    @pl.when(jnp.logical_not(giver))
    def _():
        green_copy(last, 6).wait_send()

    remote(part_sent, part_other, 5, part_sem.at[0, 0], partner).wait_send()


def f32(*shape):
    return jax.ShapeDtypeStruct(shape, jnp.float32)


def fast_device(source, green):
    size_gx = lax.axis_size("gx")
    size_gy = lax.axis_size("gy")
    size_gz = lax.axis_size("gz")
    brick_x, brick_y, brick_z = source.shape
    long_x, places, share = green.shape
    long_y = 2 * brick_y * size_gy
    long_z = 2 * brick_z * size_gz
    blocks = size_gx * size_gz
    units = places // (2 * size_gy)
    group = LANES // brick_z
    rows = brick_x // group // CHUNKS
    quarter = long_x // 4
    y_tab, y_back = y_tables(long_y, blocks, units, 1.0 / (long_x * long_z))
    x_tab, z_tab = x_table(long_x, group, rows), z_table(long_z, 2)
    flat = lambda table: table.reshape(-1, 2 * share)
    y_both = np.concatenate([y_tab, y_back], axis=3)
    tables = np.concatenate([flat(x_tab), flat(z_tab), flat(y_both)])
    each = units // PARTS
    plane = (PARTS * CHUNKS, blocks, 2 * each * rows, LANES)
    vmem = lambda *shape: pltpu.VMEM(shape, jnp.float32)
    half = lambda *shape: pltpu.VMEM(shape, jnp.bfloat16)
    raw = (CHUNKS, rows, brick_y, LANES)
    slots = (units, 4, quarter, share)
    result = pl.pallas_call(
        functools.partial(whole_kernel, size_gx, size_gz, units),
        out_shape=pltpu.VMEM((brick_x, brick_z, brick_y), jnp.float32),
        in_specs=[pl.BlockSpec(memory_space=pltpu.HBM)] * 3,
        out_specs=pl.BlockSpec(memory_space=pltpu.VMEM),
        scratch_shapes=[
            vmem(brick_x, brick_z, brick_y),
            vmem(long_x * places, share),
            half(*flat(y_both[0]).shape),
            half(*flat(x_tab).shape),
            half(8, 2 * quarter, 2 * quarter),
            half(*flat(z_tab).shape),
            half(4, long_z, 2 * share),
            half(4, long_z, 2 * share),
            vmem(*raw),
            vmem(*raw),
            vmem(*slots),
            vmem(*slots),
            vmem(*slots),
            vmem(*slots[1:]),
            vmem(*slots[1:]),
            vmem(*plane),
            vmem(*plane),
            vmem(*plane),
            vmem(*plane),
            vmem(each, long_x, LANES),
            vmem(long_x, LANES),
            vmem(2, long_x, 2 * share),
            vmem(*raw),
            vmem(*raw),
            vmem(*raw),
            pltpu.SemaphoreType.DMA((CHUNKS + 4,)),
            pltpu.SemaphoreType.DMA((7,)),
            pltpu.SemaphoreType.DMA((CHUNKS, rows)),
            pltpu.SemaphoreType.DMA((units + 1,)),
            pltpu.SemaphoreType.DMA((PARTS, CHUNKS)),
            pltpu.SemaphoreType.DMA((PARTS, CHUNKS)),
            pltpu.SemaphoreType.DMA((CHUNKS, rows)),
        ],
        compiler_params=pltpu.CompilerParams(
            vmem_limit_bytes=VMEM_BYTES, collective_id=0, has_side_effects=True
        ),
    )(jnp.swapaxes(source, 1, 2), green.reshape(long_x * places, share), tables)
    return jnp.swapaxes(result, 1, 2)


def fits(sizes, source, green):
    brick_x, brick_y, brick_z = source.shape
    units = green.shape[1] // (2 * sizes["gy"])
    return (
        brick_z * sizes["gz"] == LANES
        and green.shape[2] == LANES
        and sizes["gx"] * brick_x == 2 * LANES
        and brick_y * sizes["gy"] == LANES
        and brick_x * brick_z == 2 * CHUNKS * LANES
        and units == 2 * PARTS
        and sizes["gy"] == 2
    )


def phase_table(row_index, column_index, length):
    phase_index = row_index[:, None] * column_index[None, :] % length
    angles = phase_index.astype(jnp.float32) * (2.0 * math.pi / length)
    return (jnp.cos(angles), jnp.sin(angles))


def pair_frequency(position, length):
    unit_index = position // 2
    member = position % 2
    return jnp.where(
        unit_index == 0,
        member * (length // 2),
        jnp.where(member == 0, unit_index, length - unit_index),
    )


def product(form, left, table):
    return jnp.einsum(form, left, table, precision=lax.Precision.HIGHEST)


def mirror_plane(field, first_block):
    flipped = jnp.roll(jnp.flip(field, 1), 1, 1)
    count_y, count_x = field.shape
    swapped = flipped.reshape(count_y // 2, 2, count_x)[:, ::-1, :].reshape(count_y, count_x)
    local_row = lax.iota(jnp.int32, count_y)
    keep_unit = jnp.logical_and(first_block, local_row < 2)
    return jnp.where(keep_unit[:, None], flipped, swapped)


def per_device(source, green):
    size_gx = lax.axis_size("gx")
    size_gy = lax.axis_size("gy")
    size_gz = lax.axis_size("gz")
    brick_x, brick_y, brick_z = source.shape
    if fits({"gx": size_gx, "gy": size_gy, "gz": size_gz}, source, green):
        return fast_device(source, green)
    grid_x = brick_x * size_gx
    grid_y = brick_y * size_gy
    grid_z = brick_z * size_gz
    long_x = 2 * grid_x
    long_y = 2 * grid_y
    long_z = 2 * grid_z
    cell_z = lax.iota(jnp.int32, grid_z)
    parity_sign = (1 - 2 * (cell_z % 2)).astype(jnp.float32)
    z_lines = lax.all_to_all(source, "gz", split_axis=0, concat_axis=2, tiled=True)
    kept_freq = lax.iota(jnp.int32, long_z // 2)
    z_cos, z_sin = phase_table(cell_z, kept_freq, long_z)
    z_sin = jnp.where(kept_freq[None, :] == 0, -parity_sign[:, None], z_sin)
    z_real = product("abn,nk->abk", z_lines, z_cos)
    z_imag = -product("abn,nk->abk", z_lines, z_sin)
    y_real, y_imag = (
        lax.all_to_all(z_real, "gy", split_axis=2, concat_axis=1, tiled=True),
        lax.all_to_all(z_imag, "gy", split_axis=2, concat_axis=1, tiled=True),
    )
    y_cos, y_sin = phase_table(
        lax.iota(jnp.int32, grid_y), pair_frequency(lax.iota(jnp.int32, long_y), long_y), long_y
    )
    fy_real = product("ayc,yk->ack", y_real, y_cos) + product("ayc,yk->ack", y_imag, y_sin)
    fy_imag = product("ayc,yk->ack", y_imag, y_cos) - product("ayc,yk->ack", y_real, y_sin)
    x_real, x_imag = (
        lax.all_to_all(fy_real, ("gx", "gz"), split_axis=2, concat_axis=0, tiled=True),
        lax.all_to_all(fy_imag, ("gx", "gz"), split_axis=2, concat_axis=0, tiled=True),
    )
    x_rows = lax.iota(jnp.int32, grid_x)
    x_cos, x_sin = phase_table(x_rows, lax.iota(jnp.int32, long_x), long_x)
    full_real = product("xck,xj->ckj", x_real, x_cos) + product("xck,xj->ckj", x_imag, x_sin)
    full_imag = product("xck,xj->ckj", x_imag, x_cos) - product("xck,xj->ckj", x_real, x_sin)
    kept_green = jnp.transpose(green[:, :, 0::2], (2, 1, 0))
    nyquist_green = jnp.transpose(green[:, :, 1], (1, 0))
    prod_real = kept_green * full_real
    prod_imag = kept_green * full_imag
    first_block = lax.axis_index("gx") * size_gz + lax.axis_index("gz") == 0
    first_slab = lax.axis_index("gy") == 0
    base_real = full_real[0]
    base_imag = full_imag[0]
    mirror_real = mirror_plane(base_real, first_block)
    mirror_imag = mirror_plane(base_imag, first_block)
    zero_real = 0.5 * (base_real + mirror_real)
    zero_imag = 0.5 * (base_imag - mirror_imag)
    nyq_real = 0.5 * (base_imag + mirror_imag)
    nyq_imag = 0.5 * (mirror_real - base_real)
    zero_green = kept_green[0]
    packed_real = zero_green * zero_real - nyquist_green * nyq_imag
    packed_imag = zero_green * zero_imag + nyquist_green * nyq_real
    slot_mask = jnp.logical_and(lax.iota(jnp.int32, prod_real.shape[0]) == 0, first_slab)
    prod_real = jnp.where(slot_mask[:, None, None], packed_real[None], prod_real)
    prod_imag = jnp.where(slot_mask[:, None, None], packed_imag[None], prod_imag)
    inv_xcos, inv_xsin = phase_table(
        lax.iota(jnp.int32, long_x), lax.iota(jnp.int32, grid_x), long_x
    )
    back_real = (
        product("ckj,jx->ckx", prod_real, inv_xcos) - product("ckj,jx->ckx", prod_imag, inv_xsin)
    ) / long_x
    back_imag = (
        product("ckj,jx->ckx", prod_imag, inv_xcos) + product("ckj,jx->ckx", prod_real, inv_xsin)
    ) / long_x
    mid_real, mid_imag = (
        lax.all_to_all(back_real, ("gx", "gz"), split_axis=2, concat_axis=1, tiled=True),
        lax.all_to_all(back_imag, ("gx", "gz"), split_axis=2, concat_axis=1, tiled=True),
    )
    y_order = lax.iota(jnp.int32, long_y)
    inv_ycos, inv_ysin = phase_table(
        pair_frequency(y_order, long_y), lax.iota(jnp.int32, grid_y), long_y
    )
    half_real = (
        product("cja,jy->cay", mid_real, inv_ycos) - product("cja,jy->cay", mid_imag, inv_ysin)
    ) / long_y
    half_imag = (
        product("cja,jy->cay", mid_imag, inv_ycos) + product("cja,jy->cay", mid_real, inv_ysin)
    ) / long_y
    last_real, last_imag = (
        lax.all_to_all(half_real, "gy", split_axis=2, concat_axis=0, tiled=True),
        lax.all_to_all(half_imag, "gy", split_axis=2, concat_axis=0, tiled=True),
    )
    kept_freq = lax.iota(jnp.int32, long_z // 2)
    base_cos, base_sin = phase_table(kept_freq, cell_z, long_z)
    inv_zcos = jnp.where(kept_freq[:, None] == 0, 1.0, 2.0 * base_cos)
    inv_zsin = jnp.where(kept_freq[:, None] == 0, -parity_sign[None, :], 2.0 * base_sin)
    result = (
        product("jab,jn->abn", last_real, inv_zcos) - product("jab,jn->abn", last_imag, inv_zsin)
    ) / long_z
    return lax.all_to_all(result, "gz", split_axis=2, concat_axis=0, tiled=True)


def solution(mesh):
    step = jax.shard_map(
        per_device,
        mesh=mesh,
        in_specs=(P("gx", "gy", "gz"), P(None, ("gx", "gz"), "gy")),
        out_specs=P("gx", "gy", "gz"),
        check_vma=False,
    )
    return step
```

```python
import functools
import math

import jax
import jax.numpy as jnp
import ml_dtypes
import numpy as np
from jax import lax
from jax.experimental import pallas as pl
from jax.experimental.pallas import tpu as pltpu
from jax.sharding import PartitionSpec as P

LANES = 128
PARTS = 2
CHUNKS = 8
SENT = (3, 5, 6, 7, 8, 8, 8, 8, 8, 8)
VMEM_BYTES = 61 * 1024 * 1024


def np_halves(table):
    high = table.astype(np.float32).astype(ml_dtypes.bfloat16)
    low = (table - high.astype(np.float64)).astype(np.float32).astype(ml_dtypes.bfloat16)
    return np.stack([high, low])


def split(value):
    high = value.astype(jnp.bfloat16)
    return high, (value - high.astype(jnp.float32)).astype(jnp.bfloat16)


def mm(left, right):
    return jnp.dot(left, right, preferred_element_type=jnp.float32)


def table_left(high, low, value):
    v_high, v_low = split(value)
    both = mm(high, jnp.concatenate([v_high, v_low], axis=1))
    width = value.shape[1]
    return both[:, :width] + (both[:, width:] + mm(low, v_high))


def table_right(value, high, low):
    v_high, v_low = split(value)
    return mm(v_high, high) + (mm(v_low, high) + mm(v_high, low))


def block_swap(pieces, width):
    count = len(pieces)
    group = lax.broadcasted_iota(jnp.int32, pieces[0].shape, 1) // width
    out = []
    for c in range(count):
        total = None
        for g in range(count):
            moved = pieces[g]
            shift = (g - c) * width % LANES
            if shift:
                moved = pltpu.roll(moved, shift, 1)
            total = moved if total is None else jnp.where(group == g, moved, total)
        out.append(total)
    return out


def unit_order(units):
    each = units // PARTS
    return [*range(each)][::-1] + [*range(each, units)]


def y_tables(length_y, blocks, units, scale):
    cells = np.arange(length_y // 2)
    freq = np.arange(length_y // 2)
    angle = 2.0 * np.pi * (np.outer(freq, cells) % length_y) / length_y
    sign = 1.0 - 2.0 * (cells % 2)
    real, imag = np.cos(angle), -np.sin(angle)
    imag[0] = sign
    weight = np.where(freq == 0, 1.0, 2.0)[:, None] * (scale / length_y)
    both = np.stack([real, imag], axis=1)
    back = both * weight[:, None]

    def ordered(table):
        table = table.reshape(blocks, 2, units, 2, -1)[:, :, unit_order(units)]
        table = table.reshape(blocks, 2, PARTS, units // PARTS, 2, -1)
        return table.transpose(1, 2, 0, 3, 4, 5).reshape(2, length_y // 2, -1)

    forward = np.swapaxes(np_halves(ordered(both)), 0, 1)
    backward = np.swapaxes(np_halves(np.swapaxes(ordered(back), 1, 2)), 0, 1)
    return forward, backward


def x_table(length_x, group, rows):
    freqs = np.arange(length_x // 4)[:, None]
    place = np.arange(length_x // 2)[None, :]
    a, q, h = place % rows, place // rows % 2, place // (2 * rows) % 2
    b, block = place // (4 * rows) % group, place // (4 * rows * group)
    cells = ((2 * block + h) * rows + a) * group + b
    out = []
    for member in range(4):
        angle = 2.0 * np.pi * ((4 * freqs + member) * cells % length_x) / length_x
        c, s = np.cos(angle), np.sin(angle)
        out.append(np.concatenate([np.where(q == 0, c, s), np.where(q == 0, -s, c)], 0))
    return np_halves(np.stack(out))


def z_table(length_z, parts):
    place = np.arange(length_z)
    unit, member = place // 2, place % 2
    freq = np.where(unit == 0, member * (length_z // 2), np.where(member == 0, unit, length_z - unit))
    cells = np.arange(length_z // 2)
    rows = []
    for freqs in np.split(freq, parts):
        angle = 2.0 * np.pi * (np.outer(cells, freqs) % length_z) / length_z
        rows.append(np.concatenate([np.cos(angle), -np.sin(angle)], 1))
    return np_halves(np.stack(rows))


def expand(source, out, back):
    size = source.shape[1] // 2
    for at in range(source.shape[0] // size):
        c = source[at * size : (at + 1) * size, :size].astype(jnp.float32)
        s = source[at * size : (at + 1) * size, size:].astype(jnp.float32)
        full = jnp.concatenate(
            [jnp.concatenate([c, s], axis=1), jnp.concatenate([-s, c], axis=1)], axis=0
        )
        out[at] = full.astype(jnp.bfloat16)
        back[at] = full.T.astype(jnp.bfloat16)


def transposed(source, back):
    size = source.shape[1]
    for at in range(source.shape[0] // size):
        block = source[at * size : (at + 1) * size, :]
        back[at] = block.astype(jnp.float32).T.astype(jnp.bfloat16)


def whole_kernel(
    size_gx, size_gz, units,
    source_hbm, green_hbm, tables_hbm, out_ref,
    source, green, y_both, x_tab, x_back, z_half, z_tab, z_back,
    raw_own, raw_other, green_own, green_sent, green_other, nyquist, distant,
    f_sent, f_got, b_sent, b_got, lines, extra, spectrum, part_own, part_sent, part_other,
    local_sem, send_sem, raw_sem, green_sem, f_sem, b_sem, part_sem,
):
    gx, gy, gz = lax.axis_index("gx"), lax.axis_index("gy"), lax.axis_index("gz")
    blocks = size_gx * size_gz
    block = gx * size_gz + gz
    group = size_gz
    width = LANES // group
    rows = raw_own.shape[1]
    count_y = raw_own.shape[2]
    lines_y = 2 * count_y
    each = units // PARTS
    piece = 2 * each * rows
    share = green_own.shape[3]
    quarter = green_own.shape[2]
    half_x = 2 * quarter
    positions = 4 * units
    partner = {"gy": 1 - gy}
    lower = gy == 0
    packed = block + gy == 0

    def remote(source_at, target_at, sent, got, device):
        return pltpu.make_async_remote_copy(
            source_at, target_at, send_sem.at[sent], got,
            device_id=device, device_id_type=pl.DeviceIdType.MESH,
        )

    def plane_device(step):
        target = lax.rem(block + step, blocks)
        return target, {"gx": target // size_gz, "gz": lax.rem(target, size_gz)}

    def send_plane(sent_ref, got_ref, which, sems, part, chunk, count):
        at = pl.ds(part * CHUNKS + chunk, count)

        def body(step, _):
            target, device = plane_device(step)
            remote(
                sent_ref.at[at, target], got_ref.at[at, block], which, sems.at[part, chunk], device
            ).start()
            return 0

        lax.fori_loop(1, blocks, body, 0)
        got_ref[at, block] = sent_ref[at, block]

    def wait_plane(got_ref, which, sems, part, chunk, count):
        everything = got_ref.at[pl.ds(0, count), pl.ds(0, blocks - 1)]
        remote(everything, everything, which, sems.at[part, chunk], partner).wait_recv()

    flat = lambda ref: ref.reshape(PARTS * CHUNKS * blocks * piece, LANES)
    step_x = rows * group
    copies = [
        pltpu.make_async_copy(
            source_hbm.at[pl.ds(c * step_x, step_x)], source.at[pl.ds(c * step_x, step_x)], local_sem.at[c]
        )
        for c in range(CHUNKS)
    ]
    copies.append(pltpu.make_async_copy(green_hbm, green, local_sem.at[CHUNKS]))
    start = 0
    for n, (table, which) in enumerate(((x_tab, None), (z_half, None), (y_both, gy))):
        size = table.shape[0]
        at = start if which is None else start + which * size
        copies.append(
            pltpu.make_async_copy(
                tables_hbm.at[pl.ds(at, size), :], table, local_sem.at[CHUNKS + 1 + n]
            )
        )
        start += size
    for copy in copies:
        copy.start()

    barrier = pltpu.get_barrier_semaphore()

    def greet(step, _):
        _, device = plane_device(step)
        pl.semaphore_signal(barrier, inc=1, device_id=device, device_id_type=pl.DeviceIdType.MESH)
        return 0

    pl.semaphore_signal(barrier, inc=1, device_id=partner, device_id_type=pl.DeviceIdType.MESH)
    lax.fori_loop(1, blocks, greet, 0)

    for c in range(CHUNKS):
        copies[c].wait()
        for a in range(rows):
            at = (c * rows + a) * group
            raw_own[c, a] = jnp.concatenate([source[at + b] for b in range(group)], axis=0).T
        if c == 0:
            pl.semaphore_wait(barrier, blocks)
        for a in range(rows):
            remote(raw_own.at[c, a], raw_other.at[c, a], 0, raw_sem.at[c, a], partner).start()

    order = unit_order(units)

    def green_copy(u, sent=2):
        return remote(green_sent.at[u], green_other.at[u], sent, green_sem.at[u], partner)

    last = order.index(0)
    some = pl.ds(0, quarter // 2 + 8)
    plane_copy = remote(
        green_sent.at[last, :, some], green_other.at[last, :, some], 6, green_sem.at[last], partner
    )
    distant_copy = remote(nyquist.at[:, some], distant.at[:, some], 3, green_sem.at[units], partner)
    giver = block + (1 - gy) == 0

    def prepare(u):
        if u == 0:
            copies[CHUNKS].wait()

        def extract(m, _):
            for half, out in ((gy, green_own), (1 - gy, green_sent)):
                at = m * positions + 2 * (half * units + order[u])
                out[u, m] = green[pl.ds(at, quarter, stride=4 * positions), :]
            return 0

        lax.fori_loop(0, 4, extract, 0)
        if u != last:
            green_copy(u).start()
            return
        for m in range(4):
            nyquist[m] = green[pl.ds(m * positions + 1, quarter, stride=4 * positions), :]

        @pl.when(giver)
        def _():
            distant_copy.start()
            plane_copy.start()

        @pl.when(jnp.logical_not(giver))
        def _():
            green_copy(last, 6).start()

    copies[CHUNKS + 3].wait()

    def transform(c):
        def body(a, _):
            remote(raw_own.at[c, a], raw_other.at[c, a], 0, raw_sem.at[c, a], partner).wait_recv()
            own, other = raw_own[c, a], raw_other[c, a]
            cells = jnp.concatenate([jnp.where(lower, own, other), jnp.where(lower, other, own)], axis=0)
            freqs = table_left(y_both[:lines_y, :lines_y], y_both[lines_y:, :lines_y], cells)
            count = blocks * 2 * each
            for part in range(PARTS):
                start = (part * CHUNKS + c) * blocks * piece + a
                flat(f_sent)[pl.ds(start, count, stride=rows), :] = freqs[part * count : (part + 1) * count]
            return 0

        lax.fori_loop(0, rows, body, 0)

    for c in range(CHUNKS):
        transform(c)
        send_plane(f_sent, f_got, 1, f_sem, 0, c, 1)
        if c < units:
            prepare(c)
        elif c == units:
            copies[CHUNKS + 1].wait()
            transposed(x_tab, x_back)
        elif c == units + 1:
            copies[CHUNKS + 2].wait()
            expand(z_half, z_tab, z_back)
    for part in range(1, PARTS):
        send_plane(f_sent, f_got, 1, f_sem, part, 0, CHUNKS)

    def tiled(value):
        tiles = value.reshape(-1, 8, LANES)
        return tiles, lax.broadcasted_iota(jnp.int32, tiles.shape, 1) // rows % 2 == 0

    def turned(value):
        tiles, real = tiled(value)
        return jnp.where(real, pltpu.roll(tiles, 8 - rows, 1), -pltpu.roll(tiles, rows, 1)).reshape(value.shape)

    def chosen(where_real, where_imag):
        left, real = tiled(where_real)
        return jnp.where(real, left, tiled(where_imag)[0]).reshape(where_real.shape)

    def forward(field):
        near, far = field[:half_x], field[half_x:]
        twist = turned(far)
        out = []
        for m, cells in enumerate((near + far, near + twist, near - far, near - twist)):
            high, low = (x_tab[(4 * part + m) * half_x : (4 * part + m + 1) * half_x, :] for part in range(2))
            o = table_left(high, low, cells)
            out.append(jnp.concatenate([o[:quarter], o[quarter:]], axis=1))
        out = jnp.concatenate(out, axis=0)
        return [table_right(out, z_tab[h], z_tab[2 + h]) for h in (gy, 1 - gy)]

    def solve(field, gains_of):
        freqs = forward(field)
        for side, gain in enumerate(gains_of()):
            gain = gain.reshape(4 * quarter, share)
            spectrum[side] = jnp.concatenate([gain, gain], axis=1) * freqs[side]
        inverse = sum(
            table_right(spectrum[side], z_back[h], z_back[2 + h]) for side, h in ((0, gy), (1, 1 - gy))
        )
        cells = []
        for m in range(4):
            out = inverse[m * quarter : (m + 1) * quarter]
            both = jnp.concatenate([out[:, :LANES], out[:, LANES:]], axis=0)
            cells.append(table_left(x_back[m], x_back[4 + m], both))
        even, odd = cells[0] + cells[2], cells[1] + cells[3]
        far = (cells[0] - cells[2]) - turned(cells[1] - cells[3])
        return jnp.concatenate([even + odd, far], axis=0)

    def folded(gain):
        m = lax.broadcasted_iota(jnp.int32, gain.shape, 0)
        freq = 4 * lax.broadcasted_iota(jnp.int32, gain.shape, 1) + m
        edge = jnp.logical_or(freq == 0, freq == 2 * quarter)
        return jnp.where(edge, gain, jnp.where(freq < 2 * quarter, 2.0 * gain, 0.0))

    def unit_step(part, c):
        u = part * each + c
        here = jnp.logical_and(packed, u == last)

        def gains():
            green_copy(u).wait_recv()
            return green_own[u], green_other[u]

        def plane_gains():
            plane_copy.wait_recv()
            return green_own[last], folded(green_other[last])

        def distant_gains():
            distant_copy.wait_recv()
            return nyquist[...], folded(distant[...])

        @pl.when(jnp.logical_not(here))
        def _():
            lines[c] = solve(lines[c], gains)

        @pl.when(here)
        def _():
            field = lines[last % each]
            zero = jnp.zeros_like(field)
            extra[...] = solve(chosen(zero, field), distant_gains)
            lines[last % each] = chosen(solve(chosen(lines[last % each], zero), plane_gains), extra[...])

    def part_step(part, _):
        @pl.when(part == 0)
        def _():
            for chunk in range(CHUNKS):
                wait_plane(f_got, 1, f_sem, 0, chunk, 1)

        @pl.when(part > 0)
        def _():
            wait_plane(f_got, 1, f_sem, part, 0, CHUNKS)

        first = lax.broadcasted_iota(jnp.int32, (8, LANES), 0) < 4
        for x in range(size_gx):
            for pair in range(CHUNKS // 2):
                moved = []
                for h in range(2):
                    at = part * CHUNKS + 2 * pair + h
                    moved.append(block_swap([f_got[at, x * size_gz + g] for g in range(size_gz)], width))
                for b, (left, right) in enumerate(zip(*moved)):
                    at = ((x * CHUNKS // 2 + pair) * group + b) * 8
                    lines[0, at : at + 8] = jnp.where(first, left, pltpu.roll(right, 4, 0))
                    lines[1, at : at + 8] = jnp.where(first, pltpu.roll(left, 4, 0), right)

        def body(c, _):
            unit_step(part, c)
            return 0

        lax.fori_loop(0, each, body, 0)

        for x in range(size_gx):
            for pair in range(CHUNKS // 2):
                sides = ([], [])
                for b in range(group):
                    at = ((x * CHUNKS // 2 + pair) * group + b) * 8
                    left, right = lines[0, at : at + 8], lines[1, at : at + 8]
                    sides[0].append(jnp.where(first, left, pltpu.roll(right, 4, 0)))
                    sides[1].append(jnp.where(first, pltpu.roll(left, 4, 0), right))
                for h in range(2):
                    at = part * CHUNKS + 2 * pair + h
                    for g, moved in enumerate(block_swap(sides[h], width)):
                        b_sent[at, x * size_gz + g] = moved

        @pl.when(part < PARTS - 1)
        def _():
            send_plane(b_sent, b_got, 4, b_sem, part, 0, CHUNKS)

        @pl.when(part == PARTS - 1)
        def _():
            for chunk in range(SENT[0]):
                send_plane(b_sent, b_got, 4, b_sem, part, chunk, 1)

        return 0

    lax.fori_loop(0, PARTS, part_step, 0)

    def send_more(step):
        for chunk in range(SENT[step], SENT[step + 1]):
            send_plane(b_sent, b_got, 4, b_sem, PARTS - 1, chunk, 1)

    def part_copy(c, a):
        return remote(part_sent.at[c, a], part_other.at[c, a], 5, part_sem.at[c, a], partner)

    def invert(c):
        wait_plane(b_got, 4, b_sem, PARTS - 1, c, 1)
        send_more(c + 1)

        def body(a, _):
            count = blocks * 2 * each
            freqs = jnp.concatenate(
                [
                    flat(b_got)[pl.ds((part * CHUNKS + c) * blocks * piece + a, count, stride=rows), :]
                    for part in range(PARTS)
                ],
                axis=0,
            )
            cells = table_left(y_both[:lines_y, lines_y:], y_both[lines_y:, lines_y:], freqs)
            low, high = cells[:count_y], cells[count_y:]
            part_sent[c, a] = jnp.where(lower, high, low)
            part_own[c, a] = jnp.where(lower, low, high)
            part_copy(c, a).start()
            return 0

        lax.fori_loop(0, rows, body, 0)

    for part in range(PARTS - 1):
        wait_plane(b_got, 4, b_sem, part, 0, CHUNKS)
    send_more(0)
    for c in range(CHUNKS):
        invert(c)

    for c in range(CHUNKS):
        def finish(a, _):
            part_copy(c, a).wait_recv()
            cells = (part_own[c, a] + part_other[c, a]).T
            for b in range(group):
                out_ref[(c * rows + a) * group + b] = cells[b * width : (b + 1) * width]
            return 0

        lax.fori_loop(0, rows, finish, 0)


    remote(raw_own, raw_other, 0, raw_sem.at[0, 0], partner).wait_send()
    moved = f_sent.at[:, pl.ds(0, blocks - 1)]
    remote(moved, moved, 1, f_sem.at[0, 0], partner).wait_send()
    remote(moved, moved, 4, b_sem.at[0, 0], partner).wait_send()
    most = green_sent.at[pl.ds(0, units - 1)]
    remote(most, most, 2, green_sem.at[0], partner).wait_send()

    @pl.when(giver)
    def _():
        distant_copy.wait_send()
        plane_copy.wait_send()

    @pl.when(jnp.logical_not(giver))
    def _():
        green_copy(last, 6).wait_send()

    remote(part_sent, part_other, 5, part_sem.at[0, 0], partner).wait_send()


def f32(*shape):
    return jax.ShapeDtypeStruct(shape, jnp.float32)


def fast_device(source, green):
    size_gx = lax.axis_size("gx")
    size_gy = lax.axis_size("gy")
    size_gz = lax.axis_size("gz")
    brick_x, brick_y, brick_z = source.shape
    long_x, places, share = green.shape
    long_y = 2 * brick_y * size_gy
    long_z = 2 * brick_z * size_gz
    blocks = size_gx * size_gz
    units = places // (2 * size_gy)
    group = LANES // brick_z
    rows = brick_x // group // CHUNKS
    quarter = long_x // 4
    y_tab, y_back = y_tables(long_y, blocks, units, 1.0 / (long_x * long_z))
    x_tab, z_tab = x_table(long_x, group, rows), z_table(long_z, 2)
    flat = lambda table: table.reshape(-1, 2 * share)
    y_both = np.concatenate([y_tab, y_back], axis=3)
    tables = np.concatenate([flat(x_tab), flat(z_tab), flat(y_both)])
    each = units // PARTS
    plane = (PARTS * CHUNKS, blocks, 2 * each * rows, LANES)
    vmem = lambda *shape: pltpu.VMEM(shape, jnp.float32)
    half = lambda *shape: pltpu.VMEM(shape, jnp.bfloat16)
    raw = (CHUNKS, rows, brick_y, LANES)
    slots = (units, 4, quarter, share)
    result = pl.pallas_call(
        functools.partial(whole_kernel, size_gx, size_gz, units),
        out_shape=pltpu.VMEM((brick_x, brick_z, brick_y), jnp.float32),
        in_specs=[pl.BlockSpec(memory_space=pltpu.HBM)] * 3,
        out_specs=pl.BlockSpec(memory_space=pltpu.VMEM),
        scratch_shapes=[
            vmem(brick_x, brick_z, brick_y),
            vmem(long_x * places, share),
            half(*flat(y_both[0]).shape),
            half(*flat(x_tab).shape),
            half(8, 2 * quarter, 2 * quarter),
            half(*flat(z_tab).shape),
            half(4, long_z, 2 * share),
            half(4, long_z, 2 * share),
            vmem(*raw),
            vmem(*raw),
            vmem(*slots),
            vmem(*slots),
            vmem(*slots),
            vmem(*slots[1:]),
            vmem(*slots[1:]),
            vmem(*plane),
            vmem(*plane),
            vmem(*plane),
            vmem(*plane),
            vmem(each, long_x, LANES),
            vmem(long_x, LANES),
            vmem(2, long_x, 2 * share),
            vmem(*raw),
            vmem(*raw),
            vmem(*raw),
            pltpu.SemaphoreType.DMA((CHUNKS + 4,)),
            pltpu.SemaphoreType.DMA((7,)),
            pltpu.SemaphoreType.DMA((CHUNKS, rows)),
            pltpu.SemaphoreType.DMA((units + 1,)),
            pltpu.SemaphoreType.DMA((PARTS, CHUNKS)),
            pltpu.SemaphoreType.DMA((PARTS, CHUNKS)),
            pltpu.SemaphoreType.DMA((CHUNKS, rows)),
        ],
        compiler_params=pltpu.CompilerParams(
            vmem_limit_bytes=VMEM_BYTES, collective_id=0, has_side_effects=True
        ),
    )(jnp.swapaxes(source, 1, 2), green.reshape(long_x * places, share), tables)
    return jnp.swapaxes(result, 1, 2)


def fits(sizes, source, green):
    brick_x, brick_y, brick_z = source.shape
    units = green.shape[1] // (2 * sizes["gy"])
    return (
        brick_z * sizes["gz"] == LANES
        and green.shape[2] == LANES
        and sizes["gx"] * brick_x == 2 * LANES
        and brick_y * sizes["gy"] == LANES
        and brick_x * brick_z == 2 * CHUNKS * LANES
        and units == 2 * PARTS
        and sizes["gy"] == 2
    )


def phase_table(row_index, column_index, length):
    phase_index = row_index[:, None] * column_index[None, :] % length
    angles = phase_index.astype(jnp.float32) * (2.0 * math.pi / length)
    return (jnp.cos(angles), jnp.sin(angles))


def pair_frequency(position, length):
    unit_index = position // 2
    member = position % 2
    return jnp.where(
        unit_index == 0,
        member * (length // 2),
        jnp.where(member == 0, unit_index, length - unit_index),
    )


def product(form, left, table):
    return jnp.einsum(form, left, table, precision=lax.Precision.HIGHEST)


def mirror_plane(field, first_block):
    flipped = jnp.roll(jnp.flip(field, 1), 1, 1)
    count_y, count_x = field.shape
    swapped = flipped.reshape(count_y // 2, 2, count_x)[:, ::-1, :].reshape(count_y, count_x)
    local_row = lax.iota(jnp.int32, count_y)
    keep_unit = jnp.logical_and(first_block, local_row < 2)
    return jnp.where(keep_unit[:, None], flipped, swapped)


def per_device(source, green):
    size_gx = lax.axis_size("gx")
    size_gy = lax.axis_size("gy")
    size_gz = lax.axis_size("gz")
    brick_x, brick_y, brick_z = source.shape
    if fits({"gx": size_gx, "gy": size_gy, "gz": size_gz}, source, green):
        return fast_device(source, green)
    grid_x = brick_x * size_gx
    grid_y = brick_y * size_gy
    grid_z = brick_z * size_gz
    long_x = 2 * grid_x
    long_y = 2 * grid_y
    long_z = 2 * grid_z
    cell_z = lax.iota(jnp.int32, grid_z)
    parity_sign = (1 - 2 * (cell_z % 2)).astype(jnp.float32)
    z_lines = lax.all_to_all(source, "gz", split_axis=0, concat_axis=2, tiled=True)
    kept_freq = lax.iota(jnp.int32, long_z // 2)
    z_cos, z_sin = phase_table(cell_z, kept_freq, long_z)
    z_sin = jnp.where(kept_freq[None, :] == 0, -parity_sign[:, None], z_sin)
    z_real = product("abn,nk->abk", z_lines, z_cos)
    z_imag = -product("abn,nk->abk", z_lines, z_sin)
    y_real, y_imag = (
        lax.all_to_all(z_real, "gy", split_axis=2, concat_axis=1, tiled=True),
        lax.all_to_all(z_imag, "gy", split_axis=2, concat_axis=1, tiled=True),
    )
    y_cos, y_sin = phase_table(
        lax.iota(jnp.int32, grid_y), pair_frequency(lax.iota(jnp.int32, long_y), long_y), long_y
    )
    fy_real = product("ayc,yk->ack", y_real, y_cos) + product("ayc,yk->ack", y_imag, y_sin)
    fy_imag = product("ayc,yk->ack", y_imag, y_cos) - product("ayc,yk->ack", y_real, y_sin)
    x_real, x_imag = (
        lax.all_to_all(fy_real, ("gx", "gz"), split_axis=2, concat_axis=0, tiled=True),
        lax.all_to_all(fy_imag, ("gx", "gz"), split_axis=2, concat_axis=0, tiled=True),
    )
    x_rows = lax.iota(jnp.int32, grid_x)
    x_cos, x_sin = phase_table(x_rows, lax.iota(jnp.int32, long_x), long_x)
    full_real = product("xck,xj->ckj", x_real, x_cos) + product("xck,xj->ckj", x_imag, x_sin)
    full_imag = product("xck,xj->ckj", x_imag, x_cos) - product("xck,xj->ckj", x_real, x_sin)
    kept_green = jnp.transpose(green[:, :, 0::2], (2, 1, 0))
    nyquist_green = jnp.transpose(green[:, :, 1], (1, 0))
    prod_real = kept_green * full_real
    prod_imag = kept_green * full_imag
    first_block = lax.axis_index("gx") * size_gz + lax.axis_index("gz") == 0
    first_slab = lax.axis_index("gy") == 0
    base_real = full_real[0]
    base_imag = full_imag[0]
    mirror_real = mirror_plane(base_real, first_block)
    mirror_imag = mirror_plane(base_imag, first_block)
    zero_real = 0.5 * (base_real + mirror_real)
    zero_imag = 0.5 * (base_imag - mirror_imag)
    nyq_real = 0.5 * (base_imag + mirror_imag)
    nyq_imag = 0.5 * (mirror_real - base_real)
    zero_green = kept_green[0]
    packed_real = zero_green * zero_real - nyquist_green * nyq_imag
    packed_imag = zero_green * zero_imag + nyquist_green * nyq_real
    slot_mask = jnp.logical_and(lax.iota(jnp.int32, prod_real.shape[0]) == 0, first_slab)
    prod_real = jnp.where(slot_mask[:, None, None], packed_real[None], prod_real)
    prod_imag = jnp.where(slot_mask[:, None, None], packed_imag[None], prod_imag)
    inv_xcos, inv_xsin = phase_table(
        lax.iota(jnp.int32, long_x), lax.iota(jnp.int32, grid_x), long_x
    )
    back_real = (
        product("ckj,jx->ckx", prod_real, inv_xcos) - product("ckj,jx->ckx", prod_imag, inv_xsin)
    ) / long_x
    back_imag = (
        product("ckj,jx->ckx", prod_imag, inv_xcos) + product("ckj,jx->ckx", prod_real, inv_xsin)
    ) / long_x
    mid_real, mid_imag = (
        lax.all_to_all(back_real, ("gx", "gz"), split_axis=2, concat_axis=1, tiled=True),
        lax.all_to_all(back_imag, ("gx", "gz"), split_axis=2, concat_axis=1, tiled=True),
    )
    y_order = lax.iota(jnp.int32, long_y)
    inv_ycos, inv_ysin = phase_table(
        pair_frequency(y_order, long_y), lax.iota(jnp.int32, grid_y), long_y
    )
    half_real = (
        product("cja,jy->cay", mid_real, inv_ycos) - product("cja,jy->cay", mid_imag, inv_ysin)
    ) / long_y
    half_imag = (
        product("cja,jy->cay", mid_imag, inv_ycos) + product("cja,jy->cay", mid_real, inv_ysin)
    ) / long_y
    last_real, last_imag = (
        lax.all_to_all(half_real, "gy", split_axis=2, concat_axis=0, tiled=True),
        lax.all_to_all(half_imag, "gy", split_axis=2, concat_axis=0, tiled=True),
    )
    kept_freq = lax.iota(jnp.int32, long_z // 2)
    base_cos, base_sin = phase_table(kept_freq, cell_z, long_z)
    inv_zcos = jnp.where(kept_freq[:, None] == 0, 1.0, 2.0 * base_cos)
    inv_zsin = jnp.where(kept_freq[:, None] == 0, -parity_sign[None, :], 2.0 * base_sin)
    result = (
        product("jab,jn->abn", last_real, inv_zcos) - product("jab,jn->abn", last_imag, inv_zsin)
    ) / long_z
    return lax.all_to_all(result, "gz", split_axis=2, concat_axis=0, tiled=True)


def solution(mesh):
    step = jax.shard_map(
        per_device,
        mesh=mesh,
        in_specs=(P("gx", "gy", "gz"), P(None, ("gx", "gz"), "gy")),
        out_specs=P("gx", "gy", "gz"),
        check_vma=False,
    )
    return step
```

```python
import functools
import math

import jax
import jax.numpy as jnp
import ml_dtypes
import numpy as np
from jax import lax
from jax.experimental import pallas as pl
from jax.experimental.pallas import tpu as pltpu
from jax.sharding import PartitionSpec as P

LANES = 128
PARTS = 2
CHUNKS = 8
SENT = (3, 5, 6, 7, 8, 8, 8, 8, 8, 8)
VMEM_BYTES = 61 * 1024 * 1024


def np_halves(table):
    high = table.astype(np.float32).astype(ml_dtypes.bfloat16)
    low = (table - high.astype(np.float64)).astype(np.float32).astype(ml_dtypes.bfloat16)
    return np.stack([high, low])


def split(value):
    high = value.astype(jnp.bfloat16)
    return high, (value - high.astype(jnp.float32)).astype(jnp.bfloat16)


def mm(left, right):
    return jnp.dot(left, right, preferred_element_type=jnp.float32)


def table_left(high, low, value):
    v_high, v_low = split(value)
    both = mm(high, jnp.concatenate([v_high, v_low], axis=1))
    width = value.shape[1]
    return both[:, :width] + (both[:, width:] + mm(low, v_high))


def table_right(value, high, low):
    v_high, v_low = split(value)
    return mm(v_high, high) + (mm(v_low, high) + mm(v_high, low))


def block_swap(pieces, width):
    count = len(pieces)
    group = lax.broadcasted_iota(jnp.int32, pieces[0].shape, 1) // width
    out = []
    for c in range(count):
        total = None
        for g in range(count):
            moved = pieces[g]
            shift = (g - c) * width % LANES
            if shift:
                moved = pltpu.roll(moved, shift, 1)
            total = moved if total is None else jnp.where(group == g, moved, total)
        out.append(total)
    return out


def unit_order(units):
    each = units // PARTS
    return [*range(each)][::-1] + [*range(each, units)]


def y_tables(length_y, blocks, units, scale):
    cells = np.arange(length_y // 2)
    freq = np.arange(length_y // 2)
    angle = 2.0 * np.pi * (np.outer(freq, cells) % length_y) / length_y
    sign = 1.0 - 2.0 * (cells % 2)
    real, imag = np.cos(angle), -np.sin(angle)
    imag[0] = sign
    weight = np.where(freq == 0, 1.0, 2.0)[:, None] * (scale / length_y)
    both = np.stack([real, imag], axis=1)
    back = both * weight[:, None]

    def ordered(table):
        table = table.reshape(blocks, 2, units, 2, -1)[:, :, unit_order(units)]
        table = table.reshape(blocks, 2, PARTS, units // PARTS, 2, -1)
        return table.transpose(1, 2, 0, 3, 4, 5).reshape(2, length_y // 2, -1)

    forward = np.swapaxes(np_halves(ordered(both)), 0, 1)
    backward = np.swapaxes(np_halves(np.swapaxes(ordered(back), 1, 2)), 0, 1)
    return forward, backward


def x_table(length_x, group, rows):
    freqs = np.arange(length_x // 4)[:, None]
    place = np.arange(length_x // 2)[None, :]
    a, q, h = place % rows, place // rows % 2, place // (2 * rows) % 2
    b, block = place // (4 * rows) % group, place // (4 * rows * group)
    cells = ((2 * block + h) * rows + a) * group + b
    out = []
    for member in range(4):
        angle = 2.0 * np.pi * ((4 * freqs + member) * cells % length_x) / length_x
        c, s = np.cos(angle), np.sin(angle)
        out.append(np.concatenate([np.where(q == 0, c, s), np.where(q == 0, -s, c)], 0))
    return np_halves(np.stack(out))


def z_table(length_z, parts):
    place = np.arange(length_z)
    unit, member = place // 2, place % 2
    freq = np.where(unit == 0, member * (length_z // 2), np.where(member == 0, unit, length_z - unit))
    cells = np.arange(length_z // 2)
    rows = []
    for freqs in np.split(freq, parts):
        angle = 2.0 * np.pi * (np.outer(cells, freqs) % length_z) / length_z
        rows.append(np.concatenate([np.cos(angle), -np.sin(angle)], 1))
    return np_halves(np.stack(rows))


def expand(source, out, back):
    size = source.shape[1] // 2
    for at in range(source.shape[0] // size):
        c = source[at * size : (at + 1) * size, :size].astype(jnp.float32)
        s = source[at * size : (at + 1) * size, size:].astype(jnp.float32)
        full = jnp.concatenate(
            [jnp.concatenate([c, s], axis=1), jnp.concatenate([-s, c], axis=1)], axis=0
        )
        out[at] = full.astype(jnp.bfloat16)
        back[at] = full.T.astype(jnp.bfloat16)


def transposed(source, back):
    size = source.shape[1]
    for at in range(source.shape[0] // size):
        block = source[at * size : (at + 1) * size, :]
        back[at] = block.astype(jnp.float32).T.astype(jnp.bfloat16)


def whole_kernel(
    size_gx, size_gz, units,
    source_hbm, green_hbm, tables_hbm, out_ref,
    source, green, y_both, x_tab, x_back, z_half, z_tab, z_back,
    raw_own, raw_other, green_own, green_sent, green_other, nyquist, distant,
    f_sent, f_got, b_sent, b_got, lines, extra, spectrum, part_own, part_sent, part_other,
    local_sem, send_sem, raw_sem, green_sem, f_sem, b_sem, part_sem,
):
    gx, gy, gz = lax.axis_index("gx"), lax.axis_index("gy"), lax.axis_index("gz")
    blocks = size_gx * size_gz
    block = gx * size_gz + gz
    group = size_gz
    width = LANES // group
    rows = raw_own.shape[1]
    count_y = raw_own.shape[2]
    lines_y = 2 * count_y
    each = units // PARTS
    piece = 2 * each * rows
    share = green_own.shape[3]
    quarter = green_own.shape[2]
    half_x = 2 * quarter
    positions = 4 * units
    partner = {"gy": 1 - gy}
    lower = gy == 0
    packed = block + gy == 0

    def remote(source_at, target_at, sent, got, device):
        return pltpu.make_async_remote_copy(
            source_at, target_at, send_sem.at[sent], got,
            device_id=device, device_id_type=pl.DeviceIdType.MESH,
        )

    def plane_device(step):
        target = lax.rem(block + step, blocks)
        return target, {"gx": target // size_gz, "gz": lax.rem(target, size_gz)}

    def send_plane(sent_ref, got_ref, which, sems, part, chunk, count):
        at = pl.ds(part * CHUNKS + chunk, count)

        def body(step, _):
            target, device = plane_device(step)
            remote(
                sent_ref.at[at, target], got_ref.at[at, block], which, sems.at[part, chunk], device
            ).start()
            return 0

        lax.fori_loop(1, blocks, body, 0)
        got_ref[at, block] = sent_ref[at, block]

    def wait_plane(got_ref, which, sems, part, chunk, count):
        everything = got_ref.at[pl.ds(0, count), pl.ds(0, blocks - 1)]
        remote(everything, everything, which, sems.at[part, chunk], partner).wait_recv()

    flat = lambda ref: ref.reshape(PARTS * CHUNKS * blocks * piece, LANES)
    step_x = rows * group
    copies = [
        pltpu.make_async_copy(
            source_hbm.at[pl.ds(c * step_x, step_x)], source.at[pl.ds(c * step_x, step_x)], local_sem.at[c]
        )
        for c in range(CHUNKS)
    ]
    copies.append(pltpu.make_async_copy(green_hbm, green, local_sem.at[CHUNKS]))
    start = 0
    for n, (table, which) in enumerate(((x_tab, None), (z_half, None), (y_both, gy))):
        size = table.shape[0]
        at = start if which is None else start + which * size
        copies.append(
            pltpu.make_async_copy(
                tables_hbm.at[pl.ds(at, size), :], table, local_sem.at[CHUNKS + 1 + n]
            )
        )
        start += size
    for copy in copies:
        copy.start()

    barrier = pltpu.get_barrier_semaphore()

    def greet(step, _):
        _, device = plane_device(step)
        pl.semaphore_signal(barrier, inc=1, device_id=device, device_id_type=pl.DeviceIdType.MESH)
        return 0

    pl.semaphore_signal(barrier, inc=1, device_id=partner, device_id_type=pl.DeviceIdType.MESH)
    lax.fori_loop(1, blocks, greet, 0)

    for c in range(CHUNKS):
        copies[c].wait()
        for a in range(rows):
            at = (c * rows + a) * group
            raw_own[c, a] = jnp.concatenate([source[at + b] for b in range(group)], axis=0).T
        if c == 0:
            pl.semaphore_wait(barrier, blocks)
        for a in range(rows):
            remote(raw_own.at[c, a], raw_other.at[c, a], 0, raw_sem.at[c, a], partner).start()

    order = unit_order(units)

    def green_copy(u, sent=2):
        return remote(green_sent.at[u], green_other.at[u], sent, green_sem.at[u], partner)

    last = order.index(0)
    some = pl.ds(0, quarter // 2 + 8)
    plane_copy = remote(
        green_sent.at[last, :, some], green_other.at[last, :, some], 6, green_sem.at[last], partner
    )
    distant_copy = remote(nyquist.at[:, some], distant.at[:, some], 3, green_sem.at[units], partner)
    giver = block + (1 - gy) == 0

    def prepare(u):
        if u == 0:
            copies[CHUNKS].wait()

        def extract(m, _):
            for half, out in ((gy, green_own), (1 - gy, green_sent)):
                at = m * positions + 2 * (half * units + order[u])
                out[u, m] = green[pl.ds(at, quarter, stride=4 * positions), :]
            return 0

        lax.fori_loop(0, 4, extract, 0)
        if u != last:
            green_copy(u).start()
            return
        for m in range(4):
            nyquist[m] = green[pl.ds(m * positions + 1, quarter, stride=4 * positions), :]

        @pl.when(giver)
        def _():
            distant_copy.start()
            plane_copy.start()

        @pl.when(jnp.logical_not(giver))
        def _():
            green_copy(last, 6).start()

    copies[CHUNKS + 3].wait()

    def transform(c):
        def body(a, _):
            remote(raw_own.at[c, a], raw_other.at[c, a], 0, raw_sem.at[c, a], partner).wait_recv()
            own, other = raw_own[c, a], raw_other[c, a]
            cells = jnp.concatenate([jnp.where(lower, own, other), jnp.where(lower, other, own)], axis=0)
            freqs = table_left(y_both[:lines_y, :lines_y], y_both[lines_y:, :lines_y], cells)
            count = blocks * 2 * each
            for part in range(PARTS):
                start = (part * CHUNKS + c) * blocks * piece + a
                flat(f_sent)[pl.ds(start, count, stride=rows), :] = freqs[part * count : (part + 1) * count]
            return 0

        lax.fori_loop(0, rows, body, 0)

    for c in range(CHUNKS):
        transform(c)
        send_plane(f_sent, f_got, 1, f_sem, 0, c, 1)
        if c < units:
            prepare(c)
        elif c == units:
            copies[CHUNKS + 1].wait()
            transposed(x_tab, x_back)
        elif c == units + 1:
            copies[CHUNKS + 2].wait()
            expand(z_half, z_tab, z_back)
    for part in range(1, PARTS):
        send_plane(f_sent, f_got, 1, f_sem, part, 0, CHUNKS)

    def tiled(value):
        tiles = value.reshape(-1, 8, LANES)
        return tiles, lax.broadcasted_iota(jnp.int32, tiles.shape, 1) // rows % 2 == 0

    def turned(value):
        tiles, real = tiled(value)
        return jnp.where(real, pltpu.roll(tiles, 8 - rows, 1), -pltpu.roll(tiles, rows, 1)).reshape(value.shape)

    def chosen(where_real, where_imag):
        left, real = tiled(where_real)
        return jnp.where(real, left, tiled(where_imag)[0]).reshape(where_real.shape)

    def forward(field):
        near, far = field[:half_x], field[half_x:]
        twist = turned(far)
        out = []
        for m, cells in enumerate((near + far, near + twist, near - far, near - twist)):
            high, low = (x_tab[(4 * part + m) * half_x : (4 * part + m + 1) * half_x, :] for part in range(2))
            o = table_left(high, low, cells)
            out.append(jnp.concatenate([o[:quarter], o[quarter:]], axis=1))
        out = jnp.concatenate(out, axis=0)
        return [table_right(out, z_tab[h], z_tab[2 + h]) for h in (gy, 1 - gy)]

    def solve(field, own_gain, gain_of):
        freqs = forward(field)
        def weighted(gain, value):
            gain = gain.reshape(4 * quarter, share)
            return jnp.concatenate([gain, gain], axis=1) * value

        spectrum[0] = table_right(weighted(own_gain, freqs[0]), z_back[gy], z_back[2 + gy])
        spectrum[1] = freqs[1]
        other = weighted(gain_of(), spectrum[1])
        inverse = spectrum[0] + table_right(other, z_back[1 - gy], z_back[3 - gy])
        cells = []
        for m in range(4):
            out = inverse[m * quarter : (m + 1) * quarter]
            both = jnp.concatenate([out[:, :LANES], out[:, LANES:]], axis=0)
            cells.append(table_left(x_back[m], x_back[4 + m], both))
        even, odd = cells[0] + cells[2], cells[1] + cells[3]
        far = (cells[0] - cells[2]) - turned(cells[1] - cells[3])
        return jnp.concatenate([even + odd, far], axis=0)

    def folded(gain):
        m = lax.broadcasted_iota(jnp.int32, gain.shape, 0)
        freq = 4 * lax.broadcasted_iota(jnp.int32, gain.shape, 1) + m
        edge = jnp.logical_or(freq == 0, freq == 2 * quarter)
        return jnp.where(edge, gain, jnp.where(freq < 2 * quarter, 2.0 * gain, 0.0))

    def unit_step(part, c):
        u = part * each + c
        here = jnp.logical_and(packed, u == last)

        def gains():
            green_copy(u).wait_recv()
            return green_other[u]

        def plane_gains():
            plane_copy.wait_recv()
            return folded(green_other[last])

        def distant_gains():
            distant_copy.wait_recv()
            return folded(distant[...])

        @pl.when(jnp.logical_not(here))
        def _():
            lines[c] = solve(lines[c], green_own[u], gains)

        @pl.when(here)
        def _():
            field = lines[last % each]
            zero = jnp.zeros_like(field)
            extra[...] = solve(chosen(zero, field), nyquist[...], distant_gains)
            again = chosen(lines[last % each], zero)
            lines[last % each] = chosen(solve(again, green_own[last], plane_gains), extra[...])

    def part_step(part, _):
        @pl.when(part == 0)
        def _():
            for chunk in range(CHUNKS):
                wait_plane(f_got, 1, f_sem, 0, chunk, 1)

        @pl.when(part > 0)
        def _():
            wait_plane(f_got, 1, f_sem, part, 0, CHUNKS)

        first = lax.broadcasted_iota(jnp.int32, (8, LANES), 0) < 4
        for x in range(size_gx):
            for pair in range(CHUNKS // 2):
                moved = []
                for h in range(2):
                    at = part * CHUNKS + 2 * pair + h
                    moved.append(block_swap([f_got[at, x * size_gz + g] for g in range(size_gz)], width))
                for b, (left, right) in enumerate(zip(*moved)):
                    at = ((x * CHUNKS // 2 + pair) * group + b) * 8
                    lines[0, at : at + 8] = jnp.where(first, left, pltpu.roll(right, 4, 0))
                    lines[1, at : at + 8] = jnp.where(first, pltpu.roll(left, 4, 0), right)

        def body(c, _):
            unit_step(part, c)
            return 0

        lax.fori_loop(0, each, body, 0)

        for x in range(size_gx):
            for pair in range(CHUNKS // 2):
                sides = ([], [])
                for b in range(group):
                    at = ((x * CHUNKS // 2 + pair) * group + b) * 8
                    left, right = lines[0, at : at + 8], lines[1, at : at + 8]
                    sides[0].append(jnp.where(first, left, pltpu.roll(right, 4, 0)))
                    sides[1].append(jnp.where(first, pltpu.roll(left, 4, 0), right))
                for h in range(2):
                    at = part * CHUNKS + 2 * pair + h
                    for g, moved in enumerate(block_swap(sides[h], width)):
                        b_sent[at, x * size_gz + g] = moved

        @pl.when(part < PARTS - 1)
        def _():
            send_plane(b_sent, b_got, 4, b_sem, part, 0, CHUNKS)

        @pl.when(part == PARTS - 1)
        def _():
            for chunk in range(SENT[0]):
                send_plane(b_sent, b_got, 4, b_sem, part, chunk, 1)

        return 0

    lax.fori_loop(0, PARTS, part_step, 0)

    def send_more(step):
        for chunk in range(SENT[step], SENT[step + 1]):
            send_plane(b_sent, b_got, 4, b_sem, PARTS - 1, chunk, 1)

    def part_copy(c, a):
        return remote(part_sent.at[c, a], part_other.at[c, a], 5, part_sem.at[c, a], partner)

    def invert(c):
        wait_plane(b_got, 4, b_sem, PARTS - 1, c, 1)
        send_more(c + 1)

        def body(a, _):
            count = blocks * 2 * each
            freqs = jnp.concatenate(
                [
                    flat(b_got)[pl.ds((part * CHUNKS + c) * blocks * piece + a, count, stride=rows), :]
                    for part in range(PARTS)
                ],
                axis=0,
            )
            cells = table_left(y_both[:lines_y, lines_y:], y_both[lines_y:, lines_y:], freqs)
            low, high = cells[:count_y], cells[count_y:]
            part_sent[c, a] = jnp.where(lower, high, low)
            part_own[c, a] = jnp.where(lower, low, high)
            part_copy(c, a).start()
            return 0

        lax.fori_loop(0, rows, body, 0)

    for part in range(PARTS - 1):
        wait_plane(b_got, 4, b_sem, part, 0, CHUNKS)
    send_more(0)
    for c in range(CHUNKS):
        invert(c)

    for c in range(CHUNKS):
        def finish(a, _):
            part_copy(c, a).wait_recv()
            cells = (part_own[c, a] + part_other[c, a]).T
            for b in range(group):
                out_ref[(c * rows + a) * group + b] = cells[b * width : (b + 1) * width]
            return 0

        lax.fori_loop(0, rows, finish, 0)


    remote(raw_own, raw_other, 0, raw_sem.at[0, 0], partner).wait_send()
    moved = f_sent.at[:, pl.ds(0, blocks - 1)]
    remote(moved, moved, 1, f_sem.at[0, 0], partner).wait_send()
    remote(moved, moved, 4, b_sem.at[0, 0], partner).wait_send()
    most = green_sent.at[pl.ds(0, units - 1)]
    remote(most, most, 2, green_sem.at[0], partner).wait_send()

    @pl.when(giver)
    def _():
        distant_copy.wait_send()
        plane_copy.wait_send()

    @pl.when(jnp.logical_not(giver))
    def _():
        green_copy(last, 6).wait_send()

    remote(part_sent, part_other, 5, part_sem.at[0, 0], partner).wait_send()


def f32(*shape):
    return jax.ShapeDtypeStruct(shape, jnp.float32)


def fast_device(source, green):
    size_gx = lax.axis_size("gx")
    size_gy = lax.axis_size("gy")
    size_gz = lax.axis_size("gz")
    brick_x, brick_y, brick_z = source.shape
    long_x, places, share = green.shape
    long_y = 2 * brick_y * size_gy
    long_z = 2 * brick_z * size_gz
    blocks = size_gx * size_gz
    units = places // (2 * size_gy)
    group = LANES // brick_z
    rows = brick_x // group // CHUNKS
    quarter = long_x // 4
    y_tab, y_back = y_tables(long_y, blocks, units, 1.0 / (long_x * long_z))
    x_tab, z_tab = x_table(long_x, group, rows), z_table(long_z, 2)
    flat = lambda table: table.reshape(-1, 2 * share)
    y_both = np.concatenate([y_tab, y_back], axis=3)
    tables = np.concatenate([flat(x_tab), flat(z_tab), flat(y_both)])
    each = units // PARTS
    plane = (PARTS * CHUNKS, blocks, 2 * each * rows, LANES)
    vmem = lambda *shape: pltpu.VMEM(shape, jnp.float32)
    half = lambda *shape: pltpu.VMEM(shape, jnp.bfloat16)
    raw = (CHUNKS, rows, brick_y, LANES)
    slots = (units, 4, quarter, share)
    result = pl.pallas_call(
        functools.partial(whole_kernel, size_gx, size_gz, units),
        out_shape=pltpu.VMEM((brick_x, brick_z, brick_y), jnp.float32),
        in_specs=[pl.BlockSpec(memory_space=pltpu.HBM)] * 3,
        out_specs=pl.BlockSpec(memory_space=pltpu.VMEM),
        scratch_shapes=[
            vmem(brick_x, brick_z, brick_y),
            vmem(long_x * places, share),
            half(*flat(y_both[0]).shape),
            half(*flat(x_tab).shape),
            half(8, 2 * quarter, 2 * quarter),
            half(*flat(z_tab).shape),
            half(4, long_z, 2 * share),
            half(4, long_z, 2 * share),
            vmem(*raw),
            vmem(*raw),
            vmem(*slots),
            vmem(*slots),
            vmem(*slots),
            vmem(*slots[1:]),
            vmem(*slots[1:]),
            vmem(*plane),
            vmem(*plane),
            vmem(*plane),
            vmem(*plane),
            vmem(each, long_x, LANES),
            vmem(long_x, LANES),
            vmem(2, long_x, 2 * share),
            vmem(*raw),
            vmem(*raw),
            vmem(*raw),
            pltpu.SemaphoreType.DMA((CHUNKS + 4,)),
            pltpu.SemaphoreType.DMA((7,)),
            pltpu.SemaphoreType.DMA((CHUNKS, rows)),
            pltpu.SemaphoreType.DMA((units + 1,)),
            pltpu.SemaphoreType.DMA((PARTS, CHUNKS)),
            pltpu.SemaphoreType.DMA((PARTS, CHUNKS)),
            pltpu.SemaphoreType.DMA((CHUNKS, rows)),
        ],
        compiler_params=pltpu.CompilerParams(
            vmem_limit_bytes=VMEM_BYTES, collective_id=0, has_side_effects=True
        ),
    )(jnp.swapaxes(source, 1, 2), green.reshape(long_x * places, share), tables)
    return jnp.swapaxes(result, 1, 2)


def fits(sizes, source, green):
    brick_x, brick_y, brick_z = source.shape
    units = green.shape[1] // (2 * sizes["gy"])
    return (
        brick_z * sizes["gz"] == LANES
        and green.shape[2] == LANES
        and sizes["gx"] * brick_x == 2 * LANES
        and brick_y * sizes["gy"] == LANES
        and brick_x * brick_z == 2 * CHUNKS * LANES
        and units == 2 * PARTS
        and sizes["gy"] == 2
    )


def phase_table(row_index, column_index, length):
    phase_index = row_index[:, None] * column_index[None, :] % length
    angles = phase_index.astype(jnp.float32) * (2.0 * math.pi / length)
    return (jnp.cos(angles), jnp.sin(angles))


def pair_frequency(position, length):
    unit_index = position // 2
    member = position % 2
    return jnp.where(
        unit_index == 0,
        member * (length // 2),
        jnp.where(member == 0, unit_index, length - unit_index),
    )


def product(form, left, table):
    return jnp.einsum(form, left, table, precision=lax.Precision.HIGHEST)


def mirror_plane(field, first_block):
    flipped = jnp.roll(jnp.flip(field, 1), 1, 1)
    count_y, count_x = field.shape
    swapped = flipped.reshape(count_y // 2, 2, count_x)[:, ::-1, :].reshape(count_y, count_x)
    local_row = lax.iota(jnp.int32, count_y)
    keep_unit = jnp.logical_and(first_block, local_row < 2)
    return jnp.where(keep_unit[:, None], flipped, swapped)


def per_device(source, green):
    size_gx = lax.axis_size("gx")
    size_gy = lax.axis_size("gy")
    size_gz = lax.axis_size("gz")
    brick_x, brick_y, brick_z = source.shape
    if fits({"gx": size_gx, "gy": size_gy, "gz": size_gz}, source, green):
        return fast_device(source, green)
    grid_x = brick_x * size_gx
    grid_y = brick_y * size_gy
    grid_z = brick_z * size_gz
    long_x = 2 * grid_x
    long_y = 2 * grid_y
    long_z = 2 * grid_z
    cell_z = lax.iota(jnp.int32, grid_z)
    parity_sign = (1 - 2 * (cell_z % 2)).astype(jnp.float32)
    z_lines = lax.all_to_all(source, "gz", split_axis=0, concat_axis=2, tiled=True)
    kept_freq = lax.iota(jnp.int32, long_z // 2)
    z_cos, z_sin = phase_table(cell_z, kept_freq, long_z)
    z_sin = jnp.where(kept_freq[None, :] == 0, -parity_sign[:, None], z_sin)
    z_real = product("abn,nk->abk", z_lines, z_cos)
    z_imag = -product("abn,nk->abk", z_lines, z_sin)
    y_real, y_imag = (
        lax.all_to_all(z_real, "gy", split_axis=2, concat_axis=1, tiled=True),
        lax.all_to_all(z_imag, "gy", split_axis=2, concat_axis=1, tiled=True),
    )
    y_cos, y_sin = phase_table(
        lax.iota(jnp.int32, grid_y), pair_frequency(lax.iota(jnp.int32, long_y), long_y), long_y
    )
    fy_real = product("ayc,yk->ack", y_real, y_cos) + product("ayc,yk->ack", y_imag, y_sin)
    fy_imag = product("ayc,yk->ack", y_imag, y_cos) - product("ayc,yk->ack", y_real, y_sin)
    x_real, x_imag = (
        lax.all_to_all(fy_real, ("gx", "gz"), split_axis=2, concat_axis=0, tiled=True),
        lax.all_to_all(fy_imag, ("gx", "gz"), split_axis=2, concat_axis=0, tiled=True),
    )
    x_rows = lax.iota(jnp.int32, grid_x)
    x_cos, x_sin = phase_table(x_rows, lax.iota(jnp.int32, long_x), long_x)
    full_real = product("xck,xj->ckj", x_real, x_cos) + product("xck,xj->ckj", x_imag, x_sin)
    full_imag = product("xck,xj->ckj", x_imag, x_cos) - product("xck,xj->ckj", x_real, x_sin)
    kept_green = jnp.transpose(green[:, :, 0::2], (2, 1, 0))
    nyquist_green = jnp.transpose(green[:, :, 1], (1, 0))
    prod_real = kept_green * full_real
    prod_imag = kept_green * full_imag
    first_block = lax.axis_index("gx") * size_gz + lax.axis_index("gz") == 0
    first_slab = lax.axis_index("gy") == 0
    base_real = full_real[0]
    base_imag = full_imag[0]
    mirror_real = mirror_plane(base_real, first_block)
    mirror_imag = mirror_plane(base_imag, first_block)
    zero_real = 0.5 * (base_real + mirror_real)
    zero_imag = 0.5 * (base_imag - mirror_imag)
    nyq_real = 0.5 * (base_imag + mirror_imag)
    nyq_imag = 0.5 * (mirror_real - base_real)
    zero_green = kept_green[0]
    packed_real = zero_green * zero_real - nyquist_green * nyq_imag
    packed_imag = zero_green * zero_imag + nyquist_green * nyq_real
    slot_mask = jnp.logical_and(lax.iota(jnp.int32, prod_real.shape[0]) == 0, first_slab)
    prod_real = jnp.where(slot_mask[:, None, None], packed_real[None], prod_real)
    prod_imag = jnp.where(slot_mask[:, None, None], packed_imag[None], prod_imag)
    inv_xcos, inv_xsin = phase_table(
        lax.iota(jnp.int32, long_x), lax.iota(jnp.int32, grid_x), long_x
    )
    back_real = (
        product("ckj,jx->ckx", prod_real, inv_xcos) - product("ckj,jx->ckx", prod_imag, inv_xsin)
    ) / long_x
    back_imag = (
        product("ckj,jx->ckx", prod_imag, inv_xcos) + product("ckj,jx->ckx", prod_real, inv_xsin)
    ) / long_x
    mid_real, mid_imag = (
        lax.all_to_all(back_real, ("gx", "gz"), split_axis=2, concat_axis=1, tiled=True),
        lax.all_to_all(back_imag, ("gx", "gz"), split_axis=2, concat_axis=1, tiled=True),
    )
    y_order = lax.iota(jnp.int32, long_y)
    inv_ycos, inv_ysin = phase_table(
        pair_frequency(y_order, long_y), lax.iota(jnp.int32, grid_y), long_y
    )
    half_real = (
        product("cja,jy->cay", mid_real, inv_ycos) - product("cja,jy->cay", mid_imag, inv_ysin)
    ) / long_y
    half_imag = (
        product("cja,jy->cay", mid_imag, inv_ycos) + product("cja,jy->cay", mid_real, inv_ysin)
    ) / long_y
    last_real, last_imag = (
        lax.all_to_all(half_real, "gy", split_axis=2, concat_axis=0, tiled=True),
        lax.all_to_all(half_imag, "gy", split_axis=2, concat_axis=0, tiled=True),
    )
    kept_freq = lax.iota(jnp.int32, long_z // 2)
    base_cos, base_sin = phase_table(kept_freq, cell_z, long_z)
    inv_zcos = jnp.where(kept_freq[:, None] == 0, 1.0, 2.0 * base_cos)
    inv_zsin = jnp.where(kept_freq[:, None] == 0, -parity_sign[None, :], 2.0 * base_sin)
    result = (
        product("jab,jn->abn", last_real, inv_zcos) - product("jab,jn->abn", last_imag, inv_zsin)
    ) / long_z
    return lax.all_to_all(result, "gz", split_axis=2, concat_axis=0, tiled=True)


def solution(mesh):
    step = jax.shard_map(
        per_device,
        mesh=mesh,
        in_specs=(P("gx", "gy", "gz"), P(None, ("gx", "gz"), "gy")),
        out_specs=P("gx", "gy", "gz"),
        check_vma=False,
    )
    return step
```
